1024 devices in a mesh: gx: 32 (over x, z_hi, core), gy: 32 (over y, z_lo).
Axes of the slice: x: 8, y: 8, z: 8 (z_hi: 2, z_lo: 4; z = z_hi * 4 + z_lo), core: 2. Of those that a mesh axis runs over, the one named last changes fastest.
Arguments:
- populations: float32 [19, 512, 16384], P(None, 'gx', 'gy'), may hold values from 0.5 to 1.5
- tracer: float32 [7, 512, 16384], P(None, 'gx', 'gy'), may hold values from 0.2 to 2
- solid_mask: int32 [512, 16384], P('gx', 'gy'), may hold values 0 or 1
- inflow: int32 [512, 16384], P('gx', 'gy'), may hold values 0 or 1
- wind_profile: float32 [3, 32], replicated, may hold values from -0.12 to 0.12
- emission: float32 [512, 16384], P('gx', 'gy'), may hold values from 0.05 to 0.5
Outputs:
- final_populations: float32 [19, 512, 16384], P(None, 'gx', 'gy')
- final_tracer: float32 [7, 512, 16384], P(None, 'gx', 'gy')
The draws below stay inside these ranges and needn't reach their ends.
All inputs are finite; a program needn't handle non-finite values. No bound on the sum of `solid_mask` or of `inflow` on one device may be relied on, other than what follows from the above.
Results may differ from the reference program's by a relative error of at most 0.0001.
Values sent between devices are 32-bit elements; how exact they have to be, the bound alone decides.
A program may use at most 32 MiB of HBM per device.

```python
import math
import jax
import jax.numpy as jnp
from jax import lax

NZ = 32
STEPS = 4
NX = 512
NY = 512


def with_ends(entries, stream_key, low, top_value):
    shape = entries.shape
    index_at = [jax.random.randint(jax.random.fold_in(stream_key, axis), (), 0, shape[axis]) for axis in range(len(shape))]
    entries = entries.at[tuple(index_at)].set(low)
    longest = shape.index(max(shape))
    index_at[longest] = (index_at[longest] + 1) % shape[longest]
    return entries.at[tuple(index_at)].set(top_value)


def shard_levels(key, dims, split, least, high):
    def one(position, blocks):
        heights = jax.random.uniform(jax.random.fold_in(jax.random.fold_in(key, 6), position), (blocks,), jnp.float32, least / len(split), high / len(split))
        return jnp.repeat(jnp.exp(heights), dims[position] // blocks).reshape((-1,) + (1,) * (len(dims) - position - 1))

    level = one(*split[0])
    for cut in split[1:]:
        level = level * one(*cut)
    return level


def setup_inputs(seed: int = 0) -> dict:
    arg_keys = jax.random.split(jax.random.key(seed), 7)
    return {
        "populations": jnp.clip(0.5 + 1.0 * jax.random.uniform(arg_keys[0], (19, NX, NY * NZ), jnp.float32) ** shard_levels(arg_keys[0], (19, NX, NY * NZ), ((1, 32), (2, 32)), -0.2, 0.2), 0.5, 1.5),
        "tracer": jnp.clip(jnp.exp(math.log(2.0) - 2.3025851 * jax.random.uniform(arg_keys[1], (7, NX, NY * NZ), jnp.float32) ** shard_levels(arg_keys[1], (7, NX, NY * NZ), ((1, 32), (2, 32)), -0.2, 0.2)), 0.2, 2.0),
        "solid_mask": with_ends((jax.random.randint(arg_keys[2], (NX, NY * NZ), 0, 5) < 1).astype(jnp.int32), jax.random.fold_in(arg_keys[2], 1), 0, 1),
        "inflow": with_ends((jax.random.randint(arg_keys[3], (NX, NY * NZ), 0, 8) < 1).astype(jnp.int32), jax.random.fold_in(arg_keys[3], 1), 0, 1),
        "wind_profile": jnp.clip(jax.random.uniform(arg_keys[4], (3, NZ), jnp.float32, -0.12, 0.12), -0.12, 0.12),
        "emission": jnp.clip(jnp.exp(math.log(0.5) - 2.3025851 * jax.random.uniform(arg_keys[5], (NX, NY * NZ), jnp.float32) ** shard_levels(arg_keys[5], (NX, NY * NZ), ((0, 32), (1, 32)), -0.2, 0.2)), 0.05, 0.5),
    }


LATTICE = ((0, 0, 0), (1, 0, 0), (-1, 0, 0), (0, 1, 0), (0, -1, 0), (0, 0, 1), (0, 0, -1), (1, 1, 0), (-1, -1, 0), (1, -1, 0), (-1, 1, 0), (1, 0, 1), (-1, 0, -1), (1, 0, -1), (-1, 0, 1), (0, 1, 1), (0, -1, -1), (0, 1, -1), (0, -1, 1))
OPPOSITE = (0, 2, 1, 4, 3, 6, 5, 8, 7, 10, 9, 12, 11, 14, 13, 16, 15, 18, 17)
WEIGHTS = (1.0 / 3.0,) + (1.0 / 18.0,) * 6 + (1.0 / 36.0,) * 12
TRACER_LATTICE = LATTICE[:7]
TRACER_OPPOSITE = OPPOSITE[:7]
TRACER_WEIGHTS = (0.25,) + (0.125,) * 6
BASE_RELAX = 0.6
SMAGORINSKY = 0.2
TRACER_RELAX = 0.7

def projection(index, speed, lattice):
    return sum((lattice[index][axis] * speed[axis] for axis in range(3) if lattice[index][axis] != 0))

def equilibrium(rate, speed, speed_sq, index):
    along = projection(index, speed, LATTICE)
    return rate + 3.0 * along + 4.5 * along * along - 1.5 * speed_sq

def collide(populations, tracer, solid_mask, inflow, wind_profile, emission):
    width = populations.shape[2]
    wind_cells = jnp.tile(wind_profile, (1, width // wind_profile.shape[1]))[:, None, :]
    normal = [populations[k] for k in range(19)]
    density = sum((WEIGHTS[k] * normal[k] for k in range(19)))
    velocity = [sum((WEIGHTS[k] * LATTICE[k][axis] * normal[k] for k in range(19) if LATTICE[k][axis] != 0)) for axis in range(3)]
    speed_sq = velocity[0] * velocity[0] + velocity[1] * velocity[1] + velocity[2] * velocity[2]
    deviation = [normal[k] - equilibrium(density, velocity, speed_sq, k) for k in range(19)]
    contraction = 0.0
    for first in range(3):
        for second in range(first, 3):
            stress = sum((WEIGHTS[k] * LATTICE[k][first] * LATTICE[k][second] * deviation[k] for k in range(19) if LATTICE[k][first] * LATTICE[k][second] != 0))
            factor = 1.0 if first == second else 2.0
            contraction = contraction + factor * stress * stress
    relax_time = 0.5 * (BASE_RELAX + jnp.sqrt(BASE_RELAX * BASE_RELAX + 18.0 * math.sqrt(2.0) * SMAGORINSKY * SMAGORINSKY * jnp.sqrt(contraction)))
    wind_sq = wind_cells[0] * wind_cells[0] + wind_cells[1] * wind_cells[1] + wind_cells[2] * wind_cells[2]
    is_solid = solid_mask == 1
    is_inflow = inflow == 1
    relaxed = []
    for k in range(19):
        held = equilibrium(1.0, wind_cells, wind_sq, k)
        fluid = normal[k] - deviation[k] / relax_time
        relaxed.append(jnp.where(is_solid, normal[OPPOSITE[k]], jnp.where(is_inflow, held, fluid)))
    amount = [tracer[k] for k in range(7)]
    concentration = sum((TRACER_WEIGHTS[k] * amount[k] for k in range(7)))
    traced = []
    for k in range(7):
        balance = concentration * (1.0 + 4.0 * projection(k, velocity, TRACER_LATTICE))
        updated = amount[k] - (amount[k] - balance) / TRACER_RELAX + emission
        traced.append(jnp.where(is_solid, amount[TRACER_OPPOSITE[k]], jnp.where(is_inflow, 0.0, updated)))
    return (jnp.stack(relaxed), jnp.stack(traced))

def stream(relaxed, lattice, opposite):
    number = relaxed.shape[0]
    lattice_grid = relaxed.reshape(number, NX, NY, NZ)
    z_index = lax.iota(jnp.int32, NZ)
    layers = []
    for k in range(number):
        step_x, step_y, step_z = lattice[k]
        shifted = jnp.roll(lattice_grid[k], (step_x, step_y, step_z), axis=(0, 1, 2))
        if step_z == 1:
            shifted = jnp.where(z_index >= 1, shifted, lattice_grid[opposite[k]])
        elif step_z == -1:
            shifted = jnp.where(z_index <= NZ - 2, shifted, lattice_grid[opposite[k]])
        layers.append(shifted)
    return jnp.stack(layers).reshape(number, NX, NY * NZ)

def reference(populations, tracer, solid_mask, inflow, wind_profile, emission):
    for iteration in range(STEPS):
        relaxed, traced = collide(populations, tracer, solid_mask, inflow, wind_profile, emission)
        populations = stream(relaxed, LATTICE, OPPOSITE)
        tracer = stream(traced, TRACER_LATTICE, TRACER_OPPOSITE)
    return (populations, tracer)
```

```python
import functools
import math

import jax
import jax.numpy as jnp
from jax import lax
from jax.experimental import pallas as pl
from jax.experimental.pallas import tpu as pltpu
from jax.sharding import PartitionSpec as P

NZ = 32
STEPS = 4
FLOW = 19
TRACE = 7
POPS = FLOW + TRACE

LATTICE = (
    (0, 0, 0),
    (1, 0, 0),
    (-1, 0, 0),
    (0, 1, 0),
    (0, -1, 0),
    (0, 0, 1),
    (0, 0, -1),
    (1, 1, 0),
    (-1, -1, 0),
    (1, -1, 0),
    (-1, 1, 0),
    (1, 0, 1),
    (-1, 0, -1),
    (1, 0, -1),
    (-1, 0, 1),
    (0, 1, 1),
    (0, -1, -1),
    (0, 1, -1),
    (0, -1, 1),
)
OPPOSITE = (0, 2, 1, 4, 3, 6, 5, 8, 7, 10, 9, 12, 11, 14, 13, 16, 15, 18, 17)
MOVES = LATTICE + LATTICE[:TRACE]
BACK = OPPOSITE + tuple(FLOW + k for k in OPPOSITE[:TRACE])
BASE_RELAX = 0.6
SMAGORINSKY = 0.2
TRACER_RELAX = 0.7

SIDES = tuple(
    tuple(k for k in range(POPS) if MOVES[k][axis] == sign)
    for axis in (0, 1)
    for sign in (1, -1)
)
NEIGHBOURS = ((1, 0), (-1, 0), (0, 1), (0, -1), (1, 1), (-1, -1), (1, -1), (-1, 1))
CORNERS = (7, 8, 9, 10)
MESH = pl.DeviceIdType.MESH


def inflow_states(wind):
    square = wind[0] * wind[0] + wind[1] * wind[1] + wind[2] * wind[2]
    held = []
    for k in range(FLOW):
        along = sum(LATTICE[k][a] * wind[a] for a in range(3) if LATTICE[k][a] != 0)
        held.append(1.0 + 3.0 * along + 4.5 * along * along - 1.5 * square)
    return held


def relax_cells(h, q, solid, inflow, emission, held):
    total = {k: h[k] + h[k + 1] for k in range(1, FLOW, 2)}
    delta = {k: h[k] - h[k + 1] for k in range(1, FLOW, 2)}
    in_xy, in_xz, in_yz = total[7] + total[9], total[11] + total[13], total[15] + total[17]
    along_x, along_y, along_z = 2.0 * total[1], 2.0 * total[3], 2.0 * total[5]
    density = (
        12.0 * h[0] + ((along_x + along_y) + along_z) + ((in_xy + in_xz) + in_yz)
    ) * (1.0 / 36.0)
    speed = [
        (2.0 * delta[1] + (delta[7] + delta[9]) + (delta[11] + delta[13])) * (1.0 / 12.0),
        (2.0 * delta[3] + (delta[7] - delta[9]) + (delta[15] + delta[17])) * (1.0 / 12.0),
        (2.0 * delta[5] + (delta[11] - delta[13]) + (delta[15] - delta[17])) * (1.0 / 12.0),
    ]
    square = [v * v for v in speed]
    third = 3.0 * density
    stress_x = 0.25 * (along_x + in_xy + in_xz) - third - square[0]
    stress_y = 0.25 * (along_y + in_xy + in_yz) - third - square[1]
    stress_z = 0.25 * (along_z + in_xz + in_yz) - third - square[2]
    stress_xy = 0.25 * (total[7] - total[9]) - speed[0] * speed[1]
    stress_xz = 0.25 * (total[11] - total[13]) - speed[0] * speed[2]
    stress_yz = 0.25 * (total[15] - total[17]) - speed[1] * speed[2]
    contraction = (
        stress_x * stress_x
        + stress_y * stress_y
        + stress_z * stress_z
        + 2.0 * (stress_xy * stress_xy + stress_xz * stress_xz + stress_yz * stress_yz)
    )
    gain = 18.0 * math.sqrt(2.0) * SMAGORINSKY * SMAGORINSKY / 9.0
    rate = 2.0 / (
        BASE_RELAX + jnp.sqrt(BASE_RELAX * BASE_RELAX + gain * jnp.sqrt(contraction))
    )
    keep = 1.0 - rate
    base = rate * (density - (square[0] + square[1] + square[2]) * (1.0 / 6.0))
    half = 0.5 * rate

    def settle(k, fluid):
        return jnp.where(solid, h[OPPOSITE[k]], jnp.where(inflow, held(k), fluid))

    relaxed = [settle(0, keep * h[0] + base)]
    for k in range(1, FLOW, 2):
        along = sum(LATTICE[k][a] * speed[a] for a in range(3) if LATTICE[k][a] != 0)
        even = base + half * along * along
        odd = rate * along
        relaxed.append(settle(k, keep * h[k] + (even + odd)))
        relaxed.append(settle(k + 1, keep * h[k + 1] + (even - odd)))

    amount = 0.25 * q[0] + 0.125 * ((q[1] + q[2]) + (q[3] + q[4]) + (q[5] + q[6]))
    share = amount * (1.0 / TRACER_RELAX)
    level = share + emission
    drift = share * (4.0 / 3.0)
    rest = 1.0 - 1.0 / TRACER_RELAX

    def trace(k, fluid):
        return jnp.where(solid, q[OPPOSITE[k]], jnp.where(inflow, 0.0, fluid))

    traced = [trace(0, rest * q[0] + level)]
    for k in range(1, TRACE, 2):
        lean = drift * speed[(k - 1) // 2]
        traced.append(trace(k, rest * q[k] + (level + lean)))
        traced.append(trace(k + 1, rest * q[k + 1] + (level - lean)))
    return relaxed, traced


def kernel(
    sizes,
    flow_in,
    trace_in,
    solid_in,
    inflow_in,
    wind_in,
    emission_in,
    flow,
    trace,
    relaxed,
    solid,
    inflow,
    wind,
    emission,
    held,
    x_send,
    x_recv,
    y_send,
    y_recv,
    c_send,
    c_recv,
    in_sem,
    send_sem,
    recv_sem,
):
    rows, width = flow.shape[1], flow.shape[2]
    chunks = width // 128
    gx, gy = lax.axis_index("gx"), lax.axis_index("gy")

    def device(side):
        step_x, step_y = NEIGHBOURS[side]
        return (
            lax.rem(gx + step_x + sizes[0], sizes[0]),
            lax.rem(gy + step_y + sizes[1], sizes[1]),
        )

    barrier = pltpu.get_barrier_semaphore()
    for side in range(8):
        pl.semaphore_signal(barrier, inc=1, device_id=device(side), device_id_type=MESH)

    loads = [
        pltpu.make_async_copy(src, dst, in_sem.at[i])
        for i, (src, dst) in enumerate(
            (
                (flow_in, flow),
                (trace_in, trace),
                (solid_in, solid),
                (inflow_in, inflow),
                (emission_in, emission),
                (wind_in, wind),
            )
        )
    ]
    for load in loads:
        load.start()
    for load in loads:
        load.wait()

    winds = [jnp.concatenate([wind[a : a + 1, :]] * (128 // NZ), axis=1) for a in range(3)]
    for k, state in enumerate(inflow_states(winds)):
        held[k] = jnp.broadcast_to(state, (8, 128))

    def state(k):
        return flow.at[k] if k < FLOW else trace.at[k - FLOW]

    def relax():
        def tile(index, carry):
            row = pl.ds(pl.multiple_of((index // chunks) * 8, 8), 8)
            lane = pl.ds(pl.multiple_of((index % chunks) * 128, 128), 128)
            h = [flow[k, row, lane] for k in range(FLOW)]
            q = [trace[k, row, lane] for k in range(TRACE)]
            settled, traced = relax_cells(
                h,
                q,
                solid[row, lane] == 1,
                inflow[row, lane] == 1,
                emission[row, lane],
                lambda k: held[k],
            )
            for k, cells in enumerate(settled + traced):
                relaxed[k, row, lane] = cells
            return carry

        lax.fori_loop(0, (rows // 8) * chunks, tile, 0)

    height = lax.broadcasted_iota(jnp.int32, (rows, width), 1) % NZ

    def wall(k):
        return 0 if MOVES[k][2] == 1 else NZ - 1

    def stream():
        for k in range(POPS):
            step_x, step_y, step_z = MOVES[k]
            cells = relaxed[k]
            by = step_y * NZ + step_z
            if by != 0:
                cells = pltpu.roll(cells, by % width, 1)
            if step_x != 0:
                cells = pltpu.roll(cells, step_x % rows, 0)
            if step_z != 0:
                cells = jnp.where(height == wall(k), relaxed[BACK[k]], cells)
            state(k)[...] = cells

    lane_group = lax.broadcasted_iota(jnp.int32, (8, 128), 1) // NZ

    def pack(step):
        for side in (0, 1):
            row = 0 if side == 0 else rows - 1
            for i, k in enumerate(SIDES[side]):
                for c in range(chunks):
                    x_send[step, side, pl.ds(i * chunks + c, 1), :] = state(k)[
                        pl.ds(row, 1), pl.ds(c * 128, 128)
                    ]
        for side in (0, 1):
            lane = 0 if side == 0 else width - 128
            group = 0 if side == 0 else 128 // NZ - 1
            pops = SIDES[2 + side]
            for part in range(3):
                columns = []
                for j in range(4):
                    if part < 2:
                        k, top = pops[j], part * 8
                    else:
                        k, top = pops[4 + j % 2], (j // 2) * 8
                    cells = state(k)[pl.ds(top, 8), pl.ds(lane, 128)]
                    by = ((j - group) * NZ) % 128
                    columns.append(pltpu.roll(cells, by, 1) if by else cells)
                cells = columns[3]
                for j in range(3):
                    cells = jnp.where(lane_group == j, columns[j], cells)
                y_send[step, side, pl.ds(part * 8, 8), :] = cells
        for i, k in enumerate(CORNERS):
            row = 0 if MOVES[k][0] == 1 else rows - 1
            lane = 0 if MOVES[k][1] == 1 else width - 128
            c_send[step, i] = state(k)[pl.ds(row, 1), pl.ds(lane, 128)]

    def copies(step):
        pairs = []
        for side in range(8):
            if side < 2:
                src, dst = x_send.at[step, side], x_recv.at[step, side]
            elif side < 4:
                src, dst = y_send.at[step, side - 2], y_recv.at[step, side - 2]
            else:
                src, dst = c_send.at[step, side - 4], c_recv.at[step, side - 4]
            pairs.append(
                pltpu.make_async_remote_copy(
                    src_ref=src,
                    dst_ref=dst,
                    send_sem=send_sem.at[step, side],
                    recv_sem=recv_sem.at[step, side],
                    device_id=device(side),
                    device_id_type=MESH,
                )
            )
        return pairs

    row_height = lax.broadcasted_iota(jnp.int32, (1, 128), 1) % NZ
    tile_height = lax.broadcasted_iota(jnp.int32, (8, 128), 1) % NZ

    def patch(step):
        for side in (0, 1):
            row = 0 if side == 0 else rows - 1
            for i, k in enumerate(SIDES[side]):
                for c in range(chunks):
                    at = (pl.ds(row, 1), pl.ds(c * 128, 128))
                    cells = x_recv[step, side, pl.ds(i * chunks + c, 1), :]
                    if MOVES[k][2] != 0:
                        cells = jnp.where(row_height == wall(k), state(k)[at], cells)
                    state(k)[at] = cells
        for side in (0, 1):
            lane = 0 if side == 0 else width - 128
            group = 0 if side == 0 else 128 // NZ - 1
            for i, k in enumerate(SIDES[2 + side]):
                for half in (0, 1):
                    if i < 4:
                        part, j = half, i
                    else:
                        part, j = 2, 2 * half + i - 4
                    cells = y_recv[step, side, pl.ds(part * 8, 8), :]
                    by = ((group - j) * NZ) % 128
                    if by:
                        cells = pltpu.roll(cells, by, 1)
                    at = (pl.ds(half * 8, 8), pl.ds(lane, 128))
                    take = lane_group == group
                    if MOVES[k][2] != 0:
                        take = take & (tile_height != wall(k))
                    state(k)[at] = jnp.where(take, cells, state(k)[at])
        for i, k in enumerate(CORNERS):
            row = 0 if MOVES[k][0] == 1 else rows - 1
            lane = 0 if MOVES[k][1] == 1 else width - 128
            group = 0 if MOVES[k][1] == 1 else 128 // NZ - 1
            at = (pl.ds(row, 1), pl.ds(lane, 128))
            take = lane_group[:1] == group
            state(k)[at] = jnp.where(take, c_recv[step, i], state(k)[at])

    def advance(step, carry):
        relax()
        stream()
        pack(step)

        @pl.when(step == 0)
        def _():
            pl.semaphore_wait(barrier, 8)

        sent = copies(step)
        for copy in sent:
            copy.start()
        for copy in sent:
            copy.wait()
        patch(step)
        return carry

    lax.fori_loop(0, STEPS, advance, 0)


def local(sizes, populations, tracer, solid_mask, inflow, wind_profile, emission):
    rows, width = solid_mask.shape
    chunks = width // 128
    anywhere = pl.BlockSpec(memory_space=pl.ANY)
    near = pl.BlockSpec(memory_space=pltpu.VMEM)
    side = (STEPS, 2, 6 * chunks, 128)
    column = (STEPS, 2, 24, 128)
    corner = (STEPS, 4, 1, 128)
    return pl.pallas_call(
        functools.partial(kernel, sizes),
        out_shape=(
            jax.ShapeDtypeStruct(populations.shape, jnp.float32),
            jax.ShapeDtypeStruct(tracer.shape, jnp.float32),
        ),
        in_specs=[anywhere] * 6,
        out_specs=(near, near),
        scratch_shapes=[
            pltpu.VMEM((POPS, rows, width), jnp.float32),
            pltpu.VMEM((rows, width), jnp.int32),
            pltpu.VMEM((rows, width), jnp.int32),
            pltpu.VMEM(wind_profile.shape, jnp.float32),
            pltpu.VMEM((rows, width), jnp.float32),
            pltpu.VMEM((FLOW, 8, 128), jnp.float32),
            pltpu.VMEM(side, jnp.float32),
            pltpu.VMEM(side, jnp.float32),
            pltpu.VMEM(column, jnp.float32),
            pltpu.VMEM(column, jnp.float32),
            pltpu.VMEM(corner, jnp.float32),
            pltpu.VMEM(corner, jnp.float32),
            pltpu.SemaphoreType.DMA((6,)),
            pltpu.SemaphoreType.DMA((STEPS, 8)),
            pltpu.SemaphoreType.DMA((STEPS, 8)),
        ],
        compiler_params=pltpu.CompilerParams(collective_id=0, has_side_effects=True),
        name="canyon",
    )(populations, tracer, solid_mask, inflow, wind_profile, emission)


def solution(mesh):
    sizes = (mesh.shape["gx"], mesh.shape["gy"])
    in_specs = (
        P(None, "gx", "gy"),
        P(None, "gx", "gy"),
        P("gx", "gy"),
        P("gx", "gy"),
        P(),
        P("gx", "gy"),
    )
    out_specs = (P(None, "gx", "gy"), P(None, "gx", "gy"))
    return jax.shard_map(
        functools.partial(local, sizes),
        mesh=mesh,
        in_specs=in_specs,
        out_specs=out_specs,
        check_vma=False,
    )
```

```python
import functools
import math

import jax
import jax.numpy as jnp
from jax import lax
from jax.experimental import pallas as pl
from jax.experimental.pallas import tpu as pltpu
from jax.sharding import PartitionSpec as P

NZ = 32
STEPS = 4
MARGIN = 128
FLOW = 19
TRACE = 7
POPS = FLOW + TRACE

LATTICE = (
    (0, 0, 0),
    (1, 0, 0),
    (-1, 0, 0),
    (0, 1, 0),
    (0, -1, 0),
    (0, 0, 1),
    (0, 0, -1),
    (1, 1, 0),
    (-1, -1, 0),
    (1, -1, 0),
    (-1, 1, 0),
    (1, 0, 1),
    (-1, 0, -1),
    (1, 0, -1),
    (-1, 0, 1),
    (0, 1, 1),
    (0, -1, -1),
    (0, 1, -1),
    (0, -1, 1),
)
OPPOSITE = (0, 2, 1, 4, 3, 6, 5, 8, 7, 10, 9, 12, 11, 14, 13, 16, 15, 18, 17)
MOVES = LATTICE + LATTICE[:TRACE]
BACK = OPPOSITE + tuple(FLOW + k for k in OPPOSITE[:TRACE])
BASE_RELAX = 0.6
SMAGORINSKY = 0.2
TRACER_RELAX = 0.7

PLANES = POPS + 3
SENDS = ((1, 0), (-1, 0), (0, 1), (0, -1), (1, 1), (-1, -1), (1, -1), (-1, 1))
MESH = pl.DeviceIdType.MESH


def layers_of(k, axis, sign):
    if k >= POPS:
        return STEPS - 1
    toward = MOVES[k][axis] * sign
    if toward > 0:
        return STEPS
    if toward == 0:
        return STEPS - 1
    return STEPS - 1 if MOVES[k][2] != 0 else STEPS - 2


def row_units(sign):
    return tuple((k, n) for k in range(PLANES) for n in range(layers_of(k, 0, sign)))


UNITS = {sign: row_units(sign) for sign in (1, -1)}
COUNT = len(UNITS[1])
COLUMN = 128 // NZ


def column_tiles(sign):
    low = sign < 0

    def place(n):
        return n if low else COLUMN - 1 - n

    full = [k for k in range(PLANES) if layers_of(k, 1, sign) == STEPS]
    three = [k for k in range(PLANES) if layers_of(k, 1, sign) == STEPS - 1]
    two = [k for k in range(PLANES) if layers_of(k, 1, sign) == STEPS - 2]
    tiles = []
    for k in full:
        tiles.append({place(n): (k, n) for n in range(STEPS)})
    while three:
        group, three = three[:4], three[4:]
        if len(group) == 4:
            for n in range(3):
                tile = {place(m): (group[n], m) for m in range(3)}
                tile[place(3)] = (group[3], n)
                tiles.append(tile)
        else:
            for k in group:
                tiles.append({place(m): (k, m) for m in range(3)})
    while two:
        group, two = two[:2], two[2:]
        tile = {place(m): (group[0], m) for m in range(2)}
        for k in group[1:]:
            tile.update({place(m + 2): (k, m) for m in range(2)})
        tiles.append(tile)
    return tiles


TILES = {sign: column_tiles(sign) for sign in (1, -1)}
TILE_COUNT = len(TILES[1])


def inflow_states(wind):
    square = wind[0] * wind[0] + wind[1] * wind[1] + wind[2] * wind[2]
    held = []
    for k in range(FLOW):
        along = sum(LATTICE[k][a] * wind[a] for a in range(3) if LATTICE[k][a] != 0)
        held.append(1.0 + 3.0 * along + 4.5 * along * along - 1.5 * square)
    return held


def relax_cells(h, q, solid, inflow, emission, held):
    total = {k: h[k] + h[k + 1] for k in range(1, FLOW, 2)}
    delta = {k: h[k] - h[k + 1] for k in range(1, FLOW, 2)}
    in_xy, in_xz, in_yz = total[7] + total[9], total[11] + total[13], total[15] + total[17]
    along_x, along_y, along_z = 2.0 * total[1], 2.0 * total[3], 2.0 * total[5]
    density = (
        12.0 * h[0] + ((along_x + along_y) + along_z) + ((in_xy + in_xz) + in_yz)
    ) * (1.0 / 36.0)
    speed = [
        (2.0 * delta[1] + (delta[7] + delta[9]) + (delta[11] + delta[13])) * (1.0 / 12.0),
        (2.0 * delta[3] + (delta[7] - delta[9]) + (delta[15] + delta[17])) * (1.0 / 12.0),
        (2.0 * delta[5] + (delta[11] - delta[13]) + (delta[15] - delta[17])) * (1.0 / 12.0),
    ]
    square = [v * v for v in speed]
    third = 3.0 * density
    stress_x = 0.25 * (along_x + in_xy + in_xz) - third - square[0]
    stress_y = 0.25 * (along_y + in_xy + in_yz) - third - square[1]
    stress_z = 0.25 * (along_z + in_xz + in_yz) - third - square[2]
    stress_xy = 0.25 * (total[7] - total[9]) - speed[0] * speed[1]
    stress_xz = 0.25 * (total[11] - total[13]) - speed[0] * speed[2]
    stress_yz = 0.25 * (total[15] - total[17]) - speed[1] * speed[2]
    contraction = (
        stress_x * stress_x
        + stress_y * stress_y
        + stress_z * stress_z
        + 2.0 * (stress_xy * stress_xy + stress_xz * stress_xz + stress_yz * stress_yz)
    )
    gain = 18.0 * math.sqrt(2.0) * SMAGORINSKY * SMAGORINSKY / 9.0
    rate = 2.0 / (
        BASE_RELAX + jnp.sqrt(BASE_RELAX * BASE_RELAX + gain * jnp.sqrt(contraction))
    )
    keep = 1.0 - rate
    base = rate * (density - (square[0] + square[1] + square[2]) * (1.0 / 6.0))
    half = 0.5 * rate

    def settle(k, fluid):
        return jnp.where(solid, h[OPPOSITE[k]], jnp.where(inflow, held(k), fluid))

    relaxed = [settle(0, keep * h[0] + base)]
    for k in range(1, FLOW, 2):
        along = sum(LATTICE[k][a] * speed[a] for a in range(3) if LATTICE[k][a] != 0)
        even = base + half * along * along
        odd = rate * along
        relaxed.append(settle(k, keep * h[k] + (even + odd)))
        relaxed.append(settle(k + 1, keep * h[k + 1] + (even - odd)))

    amount = 0.25 * q[0] + 0.125 * ((q[1] + q[2]) + (q[3] + q[4]) + (q[5] + q[6]))
    share = amount * (1.0 / TRACER_RELAX)
    level = share + emission
    drift = share * (4.0 / 3.0)
    rest = 1.0 - 1.0 / TRACER_RELAX

    def trace(k, fluid):
        return jnp.where(solid, q[OPPOSITE[k]], jnp.where(inflow, 0.0, fluid))

    traced = [trace(0, rest * q[0] + level)]
    for k in range(1, TRACE, 2):
        lean = drift * speed[(k - 1) // 2]
        traced.append(trace(k, rest * q[k] + (level + lean)))
        traced.append(trace(k + 1, rest * q[k + 1] + (level - lean)))
    return relaxed, traced


def plane_of(gx, gy):
    return lax.rem(gx // 2, 2) * 4 + lax.rem(gy, 4)


class Links:
    def __init__(self, sizes, second):
        self.gx, self.gy = lax.axis_index("gx"), lax.axis_index("gy")
        self.sizes = sizes
        here = plane_of(self.gx, self.gy)
        self.out, self.into = [], []
        for side in range(8):
            late_out = self.held_back(here, plane_of(*self.target(side)))
            late_in = self.held_back(plane_of(*self.source(side)), here)
            self.out.append(late_out == second)
            self.into.append(late_in == second)

    @staticmethod
    def held_back(source, target):
        return jnp.where((source <= 4) & (target >= 6), 1, 0)

    def at(self, step_x, step_y):
        return (
            lax.rem(self.gx + step_x + self.sizes[0], self.sizes[0]),
            lax.rem(self.gy + step_y + self.sizes[1], self.sizes[1]),
        )

    def target(self, side):
        return self.at(*SENDS[side])

    def source(self, side):
        return self.at(-SENDS[side][0], -SENDS[side][1])

    def greet(self, barrier):
        for side in range(8):

            @pl.when(self.into[side])
            def _():
                pl.semaphore_signal(
                    barrier, inc=1, device_id=self.source(side), device_id_type=MESH
                )

    def meet(self, barrier):
        count = sum(jnp.where(flag, 1, 0) for flag in self.out)

        @pl.when(count > 0)
        def _():
            pl.semaphore_wait(barrier, count)

    def copy(self, side, boxes_out, boxes_in, sems):
        if side < 2:
            kind, index = 0, side
        elif side < 4:
            kind, index = 1, side - 2
        else:
            kind, index = 2, side - 4
        return pltpu.make_async_remote_copy(
            src_ref=boxes_out[kind].at[index],
            dst_ref=boxes_in[kind].at[index],
            send_sem=sems[0].at[side],
            recv_sem=sems[1].at[side],
            device_id=self.target(side),
            device_id_type=MESH,
        )

    def send(self, sides, boxes_out, boxes_in, sems):
        for side in sides:

            @pl.when(self.out[side])
            def _():
                self.copy(side, boxes_out, boxes_in, sems).start()

    def finish(self, boxes_out, boxes_in, sems):
        for side in range(8):

            @pl.when(self.into[side])
            def _():
                self.copy(side, boxes_out, boxes_in, sems).wait_recv()

        for side in range(8):

            @pl.when(self.out[side])
            def _():
                self.copy(side, boxes_out, boxes_in, sems).wait_send()


def inflow_tiles(wind, held):
    winds = [jnp.concatenate([wind[a : a + 1, :]] * COLUMN, axis=1) for a in range(3)]
    for k, cells in enumerate(inflow_states(winds)):
        held[k] = jnp.broadcast_to(cells, (8, 128))


def exchange_first(
    sizes,
    flow_in,
    trace_in,
    solid_in,
    inflow_in,
    wind_in,
    emission_in,
    relaxed,
    x_out,
    y_out,
    c_out,
    x_got,
    y_got,
    c_got,
    held,
    flow,
    trace,
    solid,
    inflow,
    wind,
    in_sem,
    send_sem,
    recv_sem,
):
    rows, width = solid.shape
    chunks = width // 128
    links = Links(sizes, 0)
    barrier = pltpu.get_barrier_semaphore()
    links.greet(barrier)

    loads = [
        pltpu.make_async_copy(src, dst, in_sem.at[i])
        for i, (src, dst) in enumerate(
            (
                (flow_in, flow),
                (trace_in, trace),
                (solid_in, solid),
                (inflow_in, inflow),
                (emission_in, relaxed.at[PLANES - 1]),
                (wind_in, wind),
            )
        )
    ]
    for load in loads:
        load.start()
    for load in loads:
        load.wait()
    inflow_tiles(wind, held)

    def tile(index, carry):
        row = pl.ds(pl.multiple_of((index // chunks) * 8, 8), 8)
        lane = pl.ds(pl.multiple_of((index % chunks) * 128, 128), 128)
        is_solid = solid[row, lane] == 1
        is_inflow = inflow[row, lane] == 1
        settled, traced = relax_cells(
            [flow[k, row, lane] for k in range(FLOW)],
            [trace[k, row, lane] for k in range(TRACE)],
            is_solid,
            is_inflow,
            relaxed[PLANES - 1, row, lane],
            lambda k: held[k],
        )
        for k, cells in enumerate(settled + traced):
            relaxed[k, row, lane] = cells
        relaxed[POPS, row, lane] = jnp.where(is_solid, 1.0, 0.0)
        relaxed[POPS + 1, row, lane] = jnp.where(is_inflow, 1.0, 0.0)
        return carry

    lax.fori_loop(0, (rows // 8) * chunks, tile, 0)

    def layer_row(sign, n):
        return rows - 1 - n if sign > 0 else n

    boxes_out, boxes_in = (x_out, y_out, c_out), (x_got, y_got, c_got)
    sems = (send_sem, recv_sem)

    for i, (sign_x, sign_y) in enumerate(SENDS[4:]):
        lane = width - 128 if sign_y > 0 else 0
        for u, (k, n) in enumerate(UNITS[sign_x]):
            c_out[i, pl.ds(u, 1), :] = relaxed[
                k, pl.ds(layer_row(sign_x, n), 1), pl.ds(lane, 128)
            ]
    links.meet(barrier)
    links.send(range(4, 8), boxes_out, boxes_in, sems)

    for i, sign in enumerate((1, -1)):
        for u, (k, n) in enumerate(UNITS[sign]):
            for c in range(chunks):
                x_out[i, pl.ds(u * chunks + c, 1), :] = relaxed[
                    k, pl.ds(layer_row(sign, n), 1), pl.ds(c * 128, 128)
                ]
    links.send((0, 1), boxes_out, boxes_in, sems)

    group = lax.broadcasted_iota(jnp.int32, (8, 128), 1) // NZ
    for i, sign in enumerate((1, -1)):
        lane = width - 128 if sign > 0 else 0
        for t, tile_map in enumerate(TILES[sign]):
            for top in range(0, rows, 8):
                parts = {}
                for place, (k, n) in tile_map.items():
                    own = COLUMN - 1 - n if sign > 0 else n
                    parts.setdefault((k, (place - own) * NZ % 128), []).append(place)
                cells = None
                for (k, by), places in parts.items():
                    piece = relaxed[k, pl.ds(top, 8), pl.ds(lane, 128)]
                    if by:
                        piece = pltpu.roll(piece, by, 1)
                    if cells is None:
                        cells = piece
                    else:
                        take = functools.reduce(jnp.logical_or, [group == p for p in places])
                        cells = jnp.where(take, piece, cells)
                y_out[i, pl.ds(t * rows + top, 8), :] = cells
    links.send((2, 3), boxes_out, boxes_in, sems)
    links.finish(boxes_out, boxes_in, sems)


def exchange_second(
    sizes, x_out, y_out, c_out, x_got, y_got, c_got, send_sem, recv_sem
):
    links = Links(sizes, 1)
    barrier = pltpu.get_barrier_semaphore()
    boxes_out, boxes_in = (x_out, y_out, c_out), (x_got, y_got, c_got)
    sems = (send_sem, recv_sem)
    links.greet(barrier)
    links.meet(barrier)
    links.send(range(8), boxes_out, boxes_in, sems)
    links.finish(boxes_out, boxes_in, sems)


def compute(
    sizes,
    relaxed_in,
    held,
    x_one,
    y_one,
    c_one,
    x_two,
    y_two,
    c_two,
    flow,
    trace,
    grown,
    state,
):
    rows, width = flow.shape[1], flow.shape[2]
    chunks = width // 128
    tall, wide = rows + 2 * STEPS, width + 2 * MARGIN
    early = Links(sizes, 0).into

    def center(k, carry):
        grown[k, pl.ds(STEPS, rows), pl.ds(MARGIN, width)] = relaxed_in[k]
        return carry

    lax.fori_loop(0, PLANES, center, 0)

    def layer_row(sign, n):
        return STEPS - 1 - n if sign > 0 else STEPS + rows + n

    def from_either(flag, unpack, one, two):
        @pl.when(flag)
        def _():
            unpack(one)

        @pl.when(jnp.logical_not(flag))
        def _():
            unpack(two)

    for i, sign in enumerate((1, -1)):

        def rows_from(box, i=i, sign=sign):
            for u, (k, n) in enumerate(UNITS[sign]):
                for c in range(chunks):
                    grown[k, pl.ds(layer_row(sign, n), 1), pl.ds(MARGIN + c * 128, 128)] = box[
                        i, pl.ds(u * chunks + c, 1), :
                    ]

        from_either(early[i], rows_from, x_one, x_two)

    group = lax.broadcasted_iota(jnp.int32, (8, 128), 1) // NZ
    for i, sign in enumerate((1, -1)):
        lane = 0 if sign > 0 else MARGIN + width

        def columns_from(box, i=i, sign=sign, lane=lane):
            pieces = {}
            for t, tile_map in enumerate(TILES[sign]):
                for place, (k, n) in tile_map.items():
                    own = COLUMN - 1 - n if sign > 0 else n
                    pieces.setdefault(k, {}).setdefault((t, (own - place) * NZ % 128), []).append(
                        own
                    )
            for k, parts in pieces.items():
                for top in range(0, rows, 8):
                    cells = None
                    for (t, by), places in parts.items():
                        piece = box[i, pl.ds(t * rows + top, 8), :]
                        if by:
                            piece = pltpu.roll(piece, by, 1)
                        if cells is None:
                            cells = piece
                        else:
                            take = functools.reduce(jnp.logical_or, [group == p for p in places])
                            cells = jnp.where(take, piece, cells)
                    grown[k, pl.ds(STEPS + top, 8), pl.ds(lane, 128)] = cells

        from_either(early[2 + i], columns_from, y_one, y_two)

    for i, (sign_x, sign_y) in enumerate(SENDS[4:]):
        lane = 0 if sign_y > 0 else MARGIN + width

        def corner_from(box, i=i, sign_x=sign_x, lane=lane):
            for u, (k, n) in enumerate(UNITS[sign_x]):
                grown[k, pl.ds(layer_row(sign_x, n), 1), pl.ds(lane, 128)] = box[
                    i, pl.ds(u, 1), :
                ]

        from_either(early[4 + i], corner_from, c_one, c_two)

    height = lax.broadcasted_iota(jnp.int32, (tall, wide), 1) % NZ

    def passed(k, up):
        step_x, step_y, step_z = MOVES[k]
        cells = grown[k]
        by = (step_y * NZ + step_z) % wide
        if by:
            cells = pltpu.roll(cells, by, 1)
        if step_x - up:
            cells = pltpu.roll(cells, (step_x - up) % tall, 0)
        if step_z:
            back = grown[BACK[k]]
            if up:
                back = pltpu.roll(back, (-up) % tall, 0)
            cells = jnp.where(height == (0 if step_z == 1 else NZ - 1), back, cells)
        return cells

    across = wide // 128

    def tile(index, carry):
        row = pl.ds(pl.multiple_of((index // across) * 8, 8), 8)
        lane = pl.ds(pl.multiple_of((index % across) * 128, 128), 128)
        settled, traced = relax_cells(
            [state[k, row, lane] for k in range(FLOW)],
            [state[FLOW + k, row, lane] for k in range(TRACE)],
            grown[POPS, row, lane] == 1.0,
            grown[POPS + 1, row, lane] == 1.0,
            grown[POPS + 2, row, lane],
            lambda k: held[k],
        )
        for k, cells in enumerate(settled + traced):
            grown[k, row, lane] = cells
        return carry

    def step(_, carry):
        for k in range(POPS):
            state[k] = passed(k, 0)
        lax.fori_loop(0, (tall // 8) * across, tile, 0)
        return carry

    lax.fori_loop(0, STEPS - 1, step, 0)
    for k in range(POPS):
        cells = passed(k, STEPS)[:rows, MARGIN : MARGIN + width]
        if k < FLOW:
            flow[k] = cells
        else:
            trace[k - FLOW] = cells


def local(sizes, populations, tracer, solid_mask, inflow, wind_profile, emission):
    rows, width = solid_mask.shape
    chunks = width // 128
    far = pl.BlockSpec(memory_space=pltpu.HBM)
    near = pl.BlockSpec(memory_space=pltpu.VMEM)
    boxes = (
        pltpu.VMEM((2, COUNT * chunks, 128), jnp.float32),
        pltpu.VMEM((2, TILE_COUNT * rows, 128), jnp.float32),
        pltpu.VMEM((4, COUNT, 128), jnp.float32),
    )

    def held_near(arrays):
        return [pltpu.with_memory_space_constraint(a, pltpu.VMEM) for a in arrays]

    held_far = [
        pltpu.with_memory_space_constraint(a, pltpu.HBM)
        for a in (populations, tracer, solid_mask, inflow, wind_profile, emission)
    ]
    relaxed, *first, held = pl.pallas_call(
        functools.partial(exchange_first, sizes),
        out_shape=(pltpu.VMEM((PLANES, rows, width), jnp.float32),)
        + boxes
        + boxes
        + (pltpu.VMEM((FLOW, 8, 128), jnp.float32),),
        in_specs=[far] * 6,
        out_specs=(near,) * 8,
        scratch_shapes=[
            pltpu.VMEM(populations.shape, jnp.float32),
            pltpu.VMEM(tracer.shape, jnp.float32),
            pltpu.VMEM((rows, width), jnp.int32),
            pltpu.VMEM((rows, width), jnp.int32),
            pltpu.VMEM(wind_profile.shape, jnp.float32),
            pltpu.SemaphoreType.DMA((6,)),
            pltpu.SemaphoreType.DMA((8,)),
            pltpu.SemaphoreType.DMA((8,)),
        ],
        compiler_params=pltpu.CompilerParams(collective_id=0, has_side_effects=True, vmem_limit_bytes=16 << 20),
        name="first",
    )(*held_far)
    second = pl.pallas_call(
        functools.partial(exchange_second, sizes),
        out_shape=boxes,
        in_specs=[near] * 3,
        out_specs=(near,) * 3,
        scratch_shapes=[pltpu.SemaphoreType.DMA((8,)), pltpu.SemaphoreType.DMA((8,))],
        compiler_params=pltpu.CompilerParams(collective_id=1, has_side_effects=True, vmem_limit_bytes=8 << 20),
        name="second",
    )(*held_near(first[:3]))
    tall, wide = rows + 2 * STEPS, width + 2 * MARGIN
    return pl.pallas_call(
        functools.partial(compute, sizes),
        out_shape=(
            jax.ShapeDtypeStruct(populations.shape, jnp.float32),
            jax.ShapeDtypeStruct(tracer.shape, jnp.float32),
        ),
        in_specs=[near] * 8,
        out_specs=(near, near),
        scratch_shapes=[
            pltpu.VMEM((PLANES, tall, wide), jnp.float32),
            pltpu.VMEM((POPS, tall, wide), jnp.float32),
        ],
        compiler_params=pltpu.CompilerParams(vmem_limit_bytes=24 << 20),
        name="compute",
    )(*held_near([relaxed, held, *first[3:], *second]))


def solution(mesh):
    sizes = (mesh.shape["gx"], mesh.shape["gy"])
    in_specs = (
        P(None, "gx", "gy"),
        P(None, "gx", "gy"),
        P("gx", "gy"),
        P("gx", "gy"),
        P(),
        P("gx", "gy"),
    )
    out_specs = (P(None, "gx", "gy"), P(None, "gx", "gy"))
    return jax.shard_map(
        functools.partial(local, sizes),
        mesh=mesh,
        in_specs=in_specs,
        out_specs=out_specs,
        check_vma=False,
    )
```

```python
import functools
import math

import jax
import jax.numpy as jnp
from jax import lax
from jax.experimental import pallas as pl
from jax.experimental.pallas import tpu as pltpu
from jax.sharding import PartitionSpec as P

NZ = 32
STEPS = 4
FLOW = 19
TRACE = 7
POPS = FLOW + TRACE

LATTICE = (
    (0, 0, 0),
    (1, 0, 0),
    (-1, 0, 0),
    (0, 1, 0),
    (0, -1, 0),
    (0, 0, 1),
    (0, 0, -1),
    (1, 1, 0),
    (-1, -1, 0),
    (1, -1, 0),
    (-1, 1, 0),
    (1, 0, 1),
    (-1, 0, -1),
    (1, 0, -1),
    (-1, 0, 1),
    (0, 1, 1),
    (0, -1, -1),
    (0, 1, -1),
    (0, -1, 1),
)
OPPOSITE = (0, 2, 1, 4, 3, 6, 5, 8, 7, 10, 9, 12, 11, 14, 13, 16, 15, 18, 17)
MOVES = LATTICE + LATTICE[:TRACE]
BACK = OPPOSITE + tuple(FLOW + k for k in OPPOSITE[:TRACE])
BASE_RELAX = 0.6
SMAGORINSKY = 0.2
TRACER_RELAX = 0.7

PLANES = POPS + 3
DEPTH = 2
ROUNDS = STEPS // DEPTH
SENDS = ((1, 0), (-1, 0), (0, 1), (0, -1), (1, 1), (-1, -1), (1, -1), (-1, 1))
MESH = pl.DeviceIdType.MESH
GROUPS = 128 // NZ
ROW_MARGIN = 8
LANE_MARGIN = 128


def layers_of(k, axis, sign):
    if k >= POPS:
        return DEPTH - 1
    toward = MOVES[k][axis] * sign
    if toward > 0:
        return DEPTH
    if toward == 0:
        return DEPTH - 1
    return DEPTH - 1 if MOVES[k][2] != 0 else DEPTH - 2


def row_units(planes, sign):
    return [(k, n) for k in range(planes) for n in range(layers_of(k, 0, sign))]


def column_units(planes, sign):
    pairs = [k for k in range(planes) if layers_of(k, 1, sign) == DEPTH]
    singles = [k for k in range(planes) if layers_of(k, 1, sign) == DEPTH - 1]
    return [(k, n) for k in pairs for n in range(DEPTH)] + [(k, 0) for k in singles]


def corner_units(planes, sign_x, sign_y):
    units = [
        (k, n, m)
        for k in range(planes)
        for n in range(layers_of(k, 0, sign_x))
        for m in range(layers_of(k, 1, sign_y))
    ]
    near = [u for u in units if u[2] == 0]
    far = [u for u in units if u[2] == 1]
    height = -(-len(near) // 3)
    return height, [near[:height], near[height : 2 * height], near[2 * height :], far]


ROWS_OF = [len(row_units(p, 1)) for p in (PLANES, POPS)]
TILES_OF = [-(-len(column_units(p, 1)) // GROUPS) for p in (PLANES, POPS)]
CORNER_OF = [corner_units(p, 1, 1)[0] for p in (PLANES, POPS)]


def inflow_states(wind):
    square = wind[0] * wind[0] + wind[1] * wind[1] + wind[2] * wind[2]
    held = []
    for k in range(FLOW):
        along = sum(LATTICE[k][a] * wind[a] for a in range(3) if LATTICE[k][a] != 0)
        held.append(1.0 + 3.0 * along + 4.5 * along * along - 1.5 * square)
    return held


def relax_cells(h, q, solid, inflow, emission, held):
    total = {k: h[k] + h[k + 1] for k in range(1, FLOW, 2)}
    delta = {k: h[k] - h[k + 1] for k in range(1, FLOW, 2)}
    in_xy, in_xz, in_yz = total[7] + total[9], total[11] + total[13], total[15] + total[17]
    along_x, along_y, along_z = 2.0 * total[1], 2.0 * total[3], 2.0 * total[5]
    density = (
        12.0 * h[0] + ((along_x + along_y) + along_z) + ((in_xy + in_xz) + in_yz)
    ) * (1.0 / 36.0)
    speed = [
        (2.0 * delta[1] + (delta[7] + delta[9]) + (delta[11] + delta[13])) * (1.0 / 12.0),
        (2.0 * delta[3] + (delta[7] - delta[9]) + (delta[15] + delta[17])) * (1.0 / 12.0),
        (2.0 * delta[5] + (delta[11] - delta[13]) + (delta[15] - delta[17])) * (1.0 / 12.0),
    ]
    square = [v * v for v in speed]
    third = 3.0 * density
    stress_x = 0.25 * (along_x + in_xy + in_xz) - third - square[0]
    stress_y = 0.25 * (along_y + in_xy + in_yz) - third - square[1]
    stress_z = 0.25 * (along_z + in_xz + in_yz) - third - square[2]
    stress_xy = 0.25 * (total[7] - total[9]) - speed[0] * speed[1]
    stress_xz = 0.25 * (total[11] - total[13]) - speed[0] * speed[2]
    stress_yz = 0.25 * (total[15] - total[17]) - speed[1] * speed[2]
    contraction = (
        stress_x * stress_x
        + stress_y * stress_y
        + stress_z * stress_z
        + 2.0 * (stress_xy * stress_xy + stress_xz * stress_xz + stress_yz * stress_yz)
    )
    gain = 18.0 * math.sqrt(2.0) * SMAGORINSKY * SMAGORINSKY / 9.0
    rate = 2.0 / (
        BASE_RELAX + jnp.sqrt(BASE_RELAX * BASE_RELAX + gain * jnp.sqrt(contraction))
    )
    keep = 1.0 - rate
    base = rate * (density - (square[0] + square[1] + square[2]) * (1.0 / 6.0))
    half = 0.5 * rate

    def settle(k, fluid):
        return jnp.where(solid, h[OPPOSITE[k]], jnp.where(inflow, held(k), fluid))

    relaxed = [settle(0, keep * h[0] + base)]
    for k in range(1, FLOW, 2):
        along = sum(LATTICE[k][a] * speed[a] for a in range(3) if LATTICE[k][a] != 0)
        even = base + half * along * along
        odd = rate * along
        relaxed.append(settle(k, keep * h[k] + (even + odd)))
        relaxed.append(settle(k + 1, keep * h[k + 1] + (even - odd)))

    amount = 0.25 * q[0] + 0.125 * ((q[1] + q[2]) + (q[3] + q[4]) + (q[5] + q[6]))
    share = amount * (1.0 / TRACER_RELAX)
    level = share + emission
    drift = share * (4.0 / 3.0)
    rest = 1.0 - 1.0 / TRACER_RELAX

    def trace(k, fluid):
        return jnp.where(solid, q[OPPOSITE[k]], jnp.where(inflow, 0.0, fluid))

    traced = [trace(0, rest * q[0] + level)]
    for k in range(1, TRACE, 2):
        lean = drift * speed[(k - 1) // 2]
        traced.append(trace(k, rest * q[k] + (level + lean)))
        traced.append(trace(k + 1, rest * q[k + 1] + (level - lean)))
    return relaxed, traced


def exchange(
    sizes,
    flow_in,
    trace_in,
    solid_in,
    inflow_in,
    wind_in,
    emission_in,
    relaxed,
    state,
    solid,
    inflow,
    wind,
    held,
    stage,
    in_sem,
    send_sem,
    recv_sem,
    *boxes,
):
    rows, width = solid.shape
    chunks = width // 128
    tall, wide = rows + ROW_MARGIN, width + LANE_MARGIN
    gx, gy = lax.axis_index("gx"), lax.axis_index("gy")

    def device(side):
        step_x, step_y = SENDS[side]
        return (
            lax.rem(gx + step_x + sizes[0], sizes[0]),
            lax.rem(gy + step_y + sizes[1], sizes[1]),
        )

    barrier = pltpu.get_barrier_semaphore()
    for side in range(8):
        pl.semaphore_signal(barrier, inc=1, device_id=device(side), device_id_type=MESH)

    block = (slice(None), pl.ds(0, rows), pl.ds(0, width))
    loads = [
        pltpu.make_async_copy(source, target, in_sem.at[i])
        for i, (source, target) in enumerate(
            (
                (flow_in, state.at[pl.ds(0, FLOW), pl.ds(0, rows), pl.ds(0, width)]),
                (trace_in, state.at[pl.ds(FLOW, TRACE), pl.ds(0, rows), pl.ds(0, width)]),
                (solid_in, solid),
                (inflow_in, inflow),
                (emission_in, relaxed.at[PLANES - 1, pl.ds(0, rows), pl.ds(0, width)]),
                (wind_in, wind),
            )
        )
    ]
    for load in loads:
        load.start()
    for load in loads:
        load.wait()
    winds = [jnp.concatenate([wind[a : a + 1, :]] * GROUPS, axis=1) for a in range(3)]
    for k, cells in enumerate(inflow_states(winds)):
        held[k] = jnp.broadcast_to(cells, (8, 128))
    relaxed[POPS, pl.ds(0, rows), pl.ds(0, width)] = jnp.where(solid[...] == 1, 1.0, 0.0)
    relaxed[POPS + 1, pl.ds(0, rows), pl.ds(0, width)] = jnp.where(inflow[...] == 1, 1.0, 0.0)

    def relax(row_tiles, lane_tiles):
        def tile(index, carry):
            row = pl.ds(pl.multiple_of((index // lane_tiles) * 8, 8), 8)
            lane = pl.ds(pl.multiple_of((index % lane_tiles) * 128, 128), 128)
            settled, traced = relax_cells(
                [state[k, row, lane] for k in range(FLOW)],
                [state[FLOW + k, row, lane] for k in range(TRACE)],
                relaxed[POPS, row, lane] == 1.0,
                relaxed[POPS + 1, row, lane] == 1.0,
                relaxed[POPS + 2, row, lane],
                lambda k: held[k],
            )
            for k, cells in enumerate(settled + traced):
                relaxed[k, row, lane] = cells
            return carry

        lax.fori_loop(0, row_tiles * lane_tiles, tile, 0)

    group = lax.broadcasted_iota(jnp.int32, (8, 128), 1) // NZ

    def merge(pieces):
        cells = pieces[0][0]
        for piece, places in pieces[1:]:
            take = functools.reduce(jnp.logical_or, [group == p for p in places])
            cells = jnp.where(take, piece, cells)
        return cells

    def turned(piece, by):
        by = by * NZ % 128
        return pltpu.roll(piece, by, 1) if by else piece

    def pack_corners(planes, box):
        for i, (sign_x, sign_y) in enumerate(SENDS[4:]):
            lane = width - 128 if sign_y > 0 else 0
            height, places = corner_units(planes, sign_x, sign_y)
            for j, units in enumerate(places):
                for u, (k, n, m) in enumerate(units):
                    row = rows - 1 - n if sign_x > 0 else n
                    stage[i, j, pl.ds(u, 1), :] = relaxed[k, pl.ds(row, 1), pl.ds(lane, 128)]
            for top in range(0, height, 8):
                pieces = []
                for j in range(4):
                    m = 1 if j == 3 else 0
                    own = GROUPS - 1 - m if sign_y > 0 else m
                    pieces.append((turned(stage[i, j, pl.ds(top, 8), :], j - own), [j]))
                count = min(8, height - top)
                box[i, pl.ds(top, count), :] = merge(pieces)[:count]

    def pack_rows(planes, box):
        for i, sign in enumerate((1, -1)):
            for u, (k, n) in enumerate(row_units(planes, sign)):
                row = rows - 1 - n if sign > 0 else n
                for c in range(chunks):
                    box[i, pl.ds(u * chunks + c, 1), :] = relaxed[
                        k, pl.ds(row, 1), pl.ds(c * 128, 128)
                    ]

    def pack_columns(planes, box):
        for i, sign in enumerate((1, -1)):
            lane = width - 128 if sign > 0 else 0
            units = column_units(planes, sign)
            for t in range(0, len(units), GROUPS):
                parts = {}
                for place, (k, n) in enumerate(units[t : t + GROUPS]):
                    own = GROUPS - 1 - n if sign > 0 else n
                    parts.setdefault((k, place - own), []).append(place)
                for top in range(0, rows, 8):
                    box[i, pl.ds(t // GROUPS * rows + top, 8), :] = merge(
                        [
                            (turned(relaxed[k, pl.ds(top, 8), pl.ds(lane, 128)], by), places)
                            for (k, by), places in parts.items()
                        ]
                    )

    def unpack_rows(planes, box):
        for i, sign in enumerate((1, -1)):
            for u, (k, n) in enumerate(row_units(planes, sign)):
                row = tall - 1 - n if sign > 0 else rows + n
                for c in range(chunks):
                    relaxed[k, pl.ds(row, 1), pl.ds(c * 128, 128)] = box[
                        i, pl.ds(u * chunks + c, 1), :
                    ]

    def unpack_columns(planes, box):
        for top in range(0, rows, 8):
            for k in range(planes):
                parts = {}
                for i, sign in enumerate((1, -1)):
                    units = column_units(planes, sign)
                    for n in range(layers_of(k, 1, sign)):
                        u = units.index((k, n))
                        own = GROUPS - 1 - n if sign > 0 else n
                        parts.setdefault((i, u // GROUPS, own - u % GROUPS), []).append(own)
                relaxed[k, pl.ds(top, 8), pl.ds(width, 128)] = merge(
                    [
                        (turned(box[i, pl.ds(t * rows + top, 8), :], by), places)
                        for (i, t, by), places in parts.items()
                    ]
                )

    def unpack_corners(planes, box):
        for i, (sign_x, sign_y) in enumerate(SENDS[4:]):
            height, places = corner_units(planes, sign_x, sign_y)
            for j, units in enumerate(places):
                m = 1 if j == 3 else 0
                own = GROUPS - 1 - m if sign_y > 0 else m
                for top in range(0, len(units), 8):
                    count = min(8, height - top)
                    stage[i, j, pl.ds(top, count), :] = turned(
                        box[i, pl.ds(top, count), :], own - j
                    )
                for u, (k, n, _) in enumerate(units):
                    row = tall - 1 - n if sign_x > 0 else rows + n
                    at = (k, pl.ds(row, 1), pl.ds(width, 128))
                    relaxed[at] = jnp.where(
                        group[:1] == own, stage[i, j, pl.ds(u, 1), :], relaxed[at]
                    )

    height = lax.broadcasted_iota(jnp.int32, (tall, wide), 1) % NZ

    def copies(step):
        x_out, x_got, y_out, y_got, c_out, c_got = boxes[6 * step : 6 * step + 6]
        pairs = []
        for side in range(8):
            if side < 2:
                source, target = x_out.at[side], x_got.at[side]
            elif side < 4:
                source, target = y_out.at[side - 2], y_got.at[side - 2]
            else:
                source, target = c_out.at[side - 4], c_got.at[side - 4]
            pairs.append(
                pltpu.make_async_remote_copy(
                    src_ref=source,
                    dst_ref=target,
                    send_sem=send_sem.at[step, side],
                    recv_sem=recv_sem.at[step, side],
                    device_id=device(side),
                    device_id_type=MESH,
                )
            )
        return pairs

    for step in range(ROUNDS):
        planes = POPS if step else PLANES
        x_out, x_got, y_out, y_got, c_out, c_got = boxes[6 * step : 6 * step + 6]
        sent = copies(step)
        relax(rows // 8, chunks)
        pack_rows(planes, x_out)
        if step == 0:
            pl.semaphore_wait(barrier, 8)
        for side in (0, 1):
            sent[side].start()
        pack_corners(planes, c_out)
        for side in range(4, 8):
            sent[side].start()
        pack_columns(planes, y_out)
        for side in (2, 3):
            sent[side].start()
        for side in (2, 3):
            sent[side].wait_recv()
        unpack_columns(planes, y_got)
        for side in (4, 5, 6, 7):
            sent[side].wait_recv()
        unpack_corners(planes, c_got)
        for side in (0, 1):
            sent[side].wait_recv()
        unpack_rows(planes, x_got)
        for copy in sent:
            copy.wait_send()
        for k in range(POPS):
            state[k] = passed(relaxed, k, height)
        relax(tall // 8, wide // 128)
        if step < ROUNDS - 1:
            for k in range(POPS):
                state[k, pl.ds(0, rows), pl.ds(0, width)] = passed(relaxed, k, height)[
                    :rows, :width
                ]


def passed(relaxed, k, height):
    step_x, step_y, step_z = MOVES[k]
    tall, wide = height.shape
    cells = relaxed[k]
    by = (step_y * NZ + step_z) % wide
    if by:
        cells = pltpu.roll(cells, by, 1)
    if step_x:
        cells = pltpu.roll(cells, step_x % tall, 0)
    if step_z:
        cells = jnp.where(height == (0 if step_z == 1 else NZ - 1), relaxed[BACK[k]], cells)
    return cells


def finish(relaxed, flow_out, trace_out, flow, trace, out_sem):
    rows, width = flow.shape[1:]
    height = lax.broadcasted_iota(jnp.int32, relaxed.shape[1:], 1) % NZ
    writes = []
    for k in range(POPS):
        near, far, at = (flow, flow_out, k) if k < FLOW else (trace, trace_out, k - FLOW)
        near[at] = passed(relaxed, k, height)[:rows, :width]
        writes.append(pltpu.make_async_copy(near.at[at], far.at[at], out_sem.at[k]))
        if k:
            writes[k - 1].start()
    writes[POPS - 1].start()
    for write in writes:
        write.wait()


def local(sizes, populations, tracer, solid_mask, inflow, wind_profile, emission):
    rows, width = solid_mask.shape
    chunks = width // 128
    tall, wide = rows + ROW_MARGIN, width + LANE_MARGIN
    far = pl.BlockSpec(memory_space=pltpu.HBM)
    near = pl.BlockSpec(memory_space=pltpu.VMEM)
    boxes = []
    for step in range(ROUNDS):
        kind = 1 if step else 0
        for shape in (
            (2, ROWS_OF[kind] * chunks, 128),
            (2, TILES_OF[kind] * rows, 128),
            (4, CORNER_OF[kind], 128),
        ):
            boxes += [pltpu.VMEM(shape, jnp.float32)] * 2
    held_far = [
        pltpu.with_memory_space_constraint(a, pltpu.HBM)
        for a in (populations, tracer, solid_mask, inflow, wind_profile, emission)
    ]
    relaxed = pl.pallas_call(
        functools.partial(exchange, sizes),
        out_shape=pltpu.VMEM((PLANES, tall, wide), jnp.float32),
        in_specs=[far] * 6,
        out_specs=near,
        scratch_shapes=[
            pltpu.VMEM((POPS, tall, wide), jnp.float32),
            pltpu.VMEM((rows, width), jnp.int32),
            pltpu.VMEM((rows, width), jnp.int32),
            pltpu.VMEM(wind_profile.shape, jnp.float32),
            pltpu.VMEM((FLOW, 8, 128), jnp.float32),
            pltpu.VMEM((4, 4, 16, 128), jnp.float32),
            pltpu.SemaphoreType.DMA((6,)),
            pltpu.SemaphoreType.DMA((ROUNDS, 8)),
            pltpu.SemaphoreType.DMA((ROUNDS, 8)),
            *boxes,
        ],
        compiler_params=pltpu.CompilerParams(
            collective_id=0, has_side_effects=True, vmem_limit_bytes=24 << 20
        ),
        name="exchange",
    )(*held_far)
    return pl.pallas_call(
        finish,
        out_shape=(
            jax.ShapeDtypeStruct(populations.shape, jnp.float32),
            jax.ShapeDtypeStruct(tracer.shape, jnp.float32),
        ),
        in_specs=[near],
        out_specs=(far, far),
        scratch_shapes=[
            pltpu.VMEM(populations.shape, jnp.float32),
            pltpu.VMEM(tracer.shape, jnp.float32),
            pltpu.SemaphoreType.DMA((POPS,)),
        ],
        compiler_params=pltpu.CompilerParams(vmem_limit_bytes=16 << 20),
        name="finish",
    )(pltpu.with_memory_space_constraint(relaxed, pltpu.VMEM))


def solution(mesh):
    sizes = (mesh.shape["gx"], mesh.shape["gy"])
    in_specs = (
        P(None, "gx", "gy"),
        P(None, "gx", "gy"),
        P("gx", "gy"),
        P("gx", "gy"),
        P(),
        P("gx", "gy"),
    )
    out_specs = (P(None, "gx", "gy"), P(None, "gx", "gy"))
    return jax.shard_map(
        functools.partial(local, sizes),
        mesh=mesh,
        in_specs=in_specs,
        out_specs=out_specs,
        check_vma=False,
    )
```

```python
import functools
import math

import jax
import jax.numpy as jnp
from jax import lax
from jax.experimental import pallas as pl
from jax.experimental.pallas import tpu as pltpu
from jax.sharding import PartitionSpec as P

NZ = 32
STEPS = 4
FLOW = 19
TRACE = 7
POPS = FLOW + TRACE

LATTICE = (
    (0, 0, 0),
    (1, 0, 0),
    (-1, 0, 0),
    (0, 1, 0),
    (0, -1, 0),
    (0, 0, 1),
    (0, 0, -1),
    (1, 1, 0),
    (-1, -1, 0),
    (1, -1, 0),
    (-1, 1, 0),
    (1, 0, 1),
    (-1, 0, -1),
    (1, 0, -1),
    (-1, 0, 1),
    (0, 1, 1),
    (0, -1, -1),
    (0, 1, -1),
    (0, -1, 1),
)
OPPOSITE = (0, 2, 1, 4, 3, 6, 5, 8, 7, 10, 9, 12, 11, 14, 13, 16, 15, 18, 17)
MOVES = LATTICE + LATTICE[:TRACE]
BACK = OPPOSITE + tuple(FLOW + k for k in OPPOSITE[:TRACE])
BASE_RELAX = 0.6
SMAGORINSKY = 0.2
TRACER_RELAX = 0.7

PLANES = POPS + 3
DEPTH = 2
ROUNDS = STEPS // DEPTH
SENDS = ((1, 0), (-1, 0), (0, 1), (0, -1), (1, 1), (-1, -1), (1, -1), (-1, 1))
MESH = pl.DeviceIdType.MESH
GROUPS = 128 // NZ
UNROLL = 2
UNROLL_ALL = 3
ROW_MARGIN = 8
LANE_MARGIN = 128


def layers_of(k, axis, sign):
    if k >= POPS:
        return DEPTH - 1
    toward = MOVES[k][axis] * sign
    if toward > 0:
        return DEPTH
    if toward == 0:
        return DEPTH - 1
    return DEPTH - 1 if MOVES[k][2] != 0 else DEPTH - 2


def row_units(planes, sign):
    return [(k, n) for k in range(planes) for n in range(layers_of(k, 0, sign))]


def column_units(planes, sign):
    pairs = [k for k in range(planes) if layers_of(k, 1, sign) == DEPTH]
    singles = [k for k in range(planes) if layers_of(k, 1, sign) == DEPTH - 1]
    return [(k, n) for k in pairs for n in range(DEPTH)] + [(k, 0) for k in singles]


def corner_units(planes, sign_x, sign_y):
    units = [
        (k, n, m)
        for k in range(planes)
        for n in range(layers_of(k, 0, sign_x))
        for m in range(layers_of(k, 1, sign_y))
    ]
    near = [u for u in units if u[2] == 0]
    far = [u for u in units if u[2] == 1]
    height = -(-len(near) // 3)
    return height, [near[:height], near[height : 2 * height], near[2 * height :], far]


ROWS_OF = [len(row_units(p, 1)) for p in (PLANES, POPS)]
TILES_OF = [-(-len(column_units(p, 1)) // GROUPS) for p in (PLANES, POPS)]
CORNER_OF = [corner_units(p, 1, 1)[0] for p in (PLANES, POPS)]


def inflow_states(wind):
    square = wind[0] * wind[0] + wind[1] * wind[1] + wind[2] * wind[2]
    held = []
    for k in range(FLOW):
        along = sum(LATTICE[k][a] * wind[a] for a in range(3) if LATTICE[k][a] != 0)
        held.append(1.0 + 3.0 * along + 4.5 * along * along - 1.5 * square)
    return held


def relax_cells(h, q, solid, inflow, emission, held):
    total = {k: h[k] + h[k + 1] for k in range(1, FLOW, 2)}
    delta = {k: h[k] - h[k + 1] for k in range(1, FLOW, 2)}
    in_xy, in_xz, in_yz = total[7] + total[9], total[11] + total[13], total[15] + total[17]
    twice = [total[k] + total[k] for k in (1, 3, 5)]
    moment = [twice[0] + (in_xy + in_xz), twice[1] + (in_xy + in_yz), twice[2] + (in_xz + in_yz)]
    density = (12.0 * h[0] + moment[0]) + ((twice[1] + twice[2]) + in_yz)
    drive = [
        (delta[1] + delta[1]) + ((delta[7] + delta[9]) + (delta[11] + delta[13])),
        (delta[3] + delta[3]) + ((delta[7] - delta[9]) + (delta[15] + delta[17])),
        (delta[5] + delta[5]) + ((delta[11] - delta[13]) + (delta[15] - delta[17])),
    ]
    speed = [d * (1.0 / 6.0) for d in drive]
    square = [v * v for v in speed]
    cross = [speed[0] * speed[1], speed[0] * speed[2], speed[1] * speed[2]]
    third = density * (1.0 / 3.0)
    stress = [(moment[a] - third) - square[a] for a in range(3)]
    shear = [
        (total[7] - total[9]) - cross[0],
        (total[11] - total[13]) - cross[1],
        (total[15] - total[17]) - cross[2],
    ]
    sheared = (shear[0] * shear[0] + shear[1] * shear[1]) + shear[2] * shear[2]
    contraction = ((stress[0] * stress[0] + stress[1] * stress[1]) + stress[2] * stress[2]) + (
        sheared + sheared
    )
    gain = 18.0 * math.sqrt(2.0) * SMAGORINSKY * SMAGORINSKY / 36.0
    inner = BASE_RELAX * BASE_RELAX + gain * jnp.sqrt(contraction)
    half = 1.0 / (BASE_RELAX + inner * lax.rsqrt(inner))
    keep = 1.0 - (half + half)
    base = half * (
        density * (1.0 / 18.0) - ((square[0] + square[1]) + square[2]) * (1.0 / 12.0)
    )
    lean = [half * v for v in speed]
    quarter = 0.25 * half
    bend = [quarter * v for v in square]
    twist = [(0.5 * half) * v for v in cross]
    straight = [base + v for v in bend]
    slant = [straight[0] + bend[1], straight[0] + bend[2], straight[1] + bend[2]]

    def settle(k, fluid):
        return jnp.where(solid, h[OPPOSITE[k]], jnp.where(inflow, held(k), fluid))

    relaxed = [settle(0, keep * h[0] + base)]

    def pair(k, even, odd):
        relaxed.append(settle(k, keep * h[k] + (even + odd)))
        relaxed.append(settle(k + 1, keep * h[k + 1] + (even - odd)))

    for a in range(3):
        pair(2 * a + 1, straight[a], lean[a])
    for i, (a, b) in enumerate(((0, 1), (0, 2), (1, 2))):
        pair(4 * i + 7, slant[i] + twist[i], lean[a] + lean[b])
        pair(4 * i + 9, slant[i] - twist[i], lean[a] - lean[b])

    share = (0.25 / TRACER_RELAX) * q[0] + (0.125 / TRACER_RELAX) * (
        (q[1] + q[2]) + (q[3] + q[4]) + (q[5] + q[6])
    )
    level = share + emission
    drift = share * (2.0 / 3.0)
    rest = 1.0 - 1.0 / TRACER_RELAX

    def trace(k, fluid):
        return jnp.where(solid, q[OPPOSITE[k]], jnp.where(inflow, 0.0, fluid))

    traced = [trace(0, rest * q[0] + level)]
    for k in range(1, TRACE, 2):
        carried = drift * speed[(k - 1) // 2]
        traced.append(trace(k, rest * q[k] + (level + carried)))
        traced.append(trace(k + 1, rest * q[k + 1] + (level - carried)))
    return relaxed, traced


def exchange(
    sizes,
    flow_in,
    trace_in,
    solid_in,
    inflow_in,
    wind_in,
    emission_in,
    relaxed,
    state,
    solid,
    inflow,
    wind,
    held,
    stage,
    in_sem,
    send_sem,
    recv_sem,
    *boxes,
):
    rows, width = solid.shape
    chunks = width // 128
    tall, wide = rows + ROW_MARGIN, width + LANE_MARGIN
    gx, gy = lax.axis_index("gx"), lax.axis_index("gy")

    def device(side):
        step_x, step_y = SENDS[side]
        return (
            lax.rem(gx + step_x + sizes[0], sizes[0]),
            lax.rem(gy + step_y + sizes[1], sizes[1]),
        )

    barrier = pltpu.get_barrier_semaphore()
    for side in range(8):
        pl.semaphore_signal(barrier, inc=1, device_id=device(side), device_id_type=MESH)

    block = (slice(None), pl.ds(0, rows), pl.ds(0, width))
    loads = [
        pltpu.make_async_copy(source, target, in_sem.at[i])
        for i, (source, target) in enumerate(
            (
                (flow_in, state.at[pl.ds(0, FLOW), pl.ds(0, rows), pl.ds(0, width)]),
                (trace_in, state.at[pl.ds(FLOW, TRACE), pl.ds(0, rows), pl.ds(0, width)]),
                (solid_in, solid),
                (inflow_in, inflow),
                (emission_in, relaxed.at[PLANES - 1, pl.ds(0, rows), pl.ds(0, width)]),
                (wind_in, wind),
            )
        )
    ]
    for load in loads:
        load.start()
    for load in loads:
        load.wait()
    winds = [jnp.concatenate([wind[a : a + 1, :]] * GROUPS, axis=1) for a in range(3)]
    for k, cells in enumerate(inflow_states(winds)):
        held[k] = jnp.broadcast_to(cells, (8, 128))
    relaxed[POPS, pl.ds(0, rows), pl.ds(0, width)] = jnp.where(solid[...] == 1, 1.0, 0.0)
    relaxed[POPS + 1, pl.ds(0, rows), pl.ds(0, width)] = jnp.where(inflow[...] == 1, 1.0, 0.0)

    def relax_tile(row_tile, lane_tile):
        row = pl.ds(pl.multiple_of(row_tile * 8, 8), 8)
        lane = pl.ds(pl.multiple_of(lane_tile * 128, 128), 128)
        settled, traced = relax_cells(
            [state[k, row, lane] for k in range(FLOW)],
            [state[FLOW + k, row, lane] for k in range(TRACE)],
            relaxed[POPS, row, lane] == 1.0,
            relaxed[POPS + 1, row, lane] == 1.0,
            relaxed[POPS + 2, row, lane],
            lambda k: held[k],
        )
        for k, cells in enumerate(settled + traced):
            relaxed[k, row, lane] = cells

    def relax(row_tiles, lane_tiles, unroll):
        def tiles(index, carry):
            for i in range(unroll):
                at = index * unroll + i
                relax_tile(at // lane_tiles, at % lane_tiles)
            return carry

        lax.fori_loop(0, row_tiles * lane_tiles // unroll, tiles, 0)

    def relax_row(row_tile, unroll):
        def tiles(index, carry):
            for i in range(unroll):
                relax_tile(row_tile, index * unroll + i)
            return carry

        lax.fori_loop(0, chunks // unroll, tiles, 0)

    group = lax.broadcasted_iota(jnp.int32, (8, 128), 1) // NZ

    def merge(pieces):
        cells = pieces[0][0]
        for piece, places in pieces[1:]:
            take = functools.reduce(jnp.logical_or, [group == p for p in places])
            cells = jnp.where(take, piece, cells)
        return cells

    def turned(piece, by):
        by = by * NZ % 128
        return pltpu.roll(piece, by, 1) if by else piece

    def pack_corners(planes, box):
        for i, (sign_x, sign_y) in enumerate(SENDS[4:]):
            lane = width - 128 if sign_y > 0 else 0
            height, places = corner_units(planes, sign_x, sign_y)
            for j, units in enumerate(places):
                for u, (k, n, m) in enumerate(units):
                    row = rows - 1 - n if sign_x > 0 else n
                    stage[i, j, pl.ds(u, 1), :] = relaxed[k, pl.ds(row, 1), pl.ds(lane, 128)]
            for top in range(0, height, 8):
                pieces = []
                for j in range(4):
                    m = 1 if j == 3 else 0
                    own = GROUPS - 1 - m if sign_y > 0 else m
                    pieces.append((turned(stage[i, j, pl.ds(top, 8), :], j - own), [j]))
                count = min(8, height - top)
                box[i, pl.ds(top, count), :] = merge(pieces)[:count]

    def pack_rows(planes, box, i):
        sign = SENDS[i][0]
        for u, (k, n) in enumerate(row_units(planes, sign)):
            row = rows - 1 - n if sign > 0 else n
            for c in range(chunks):
                box[i, pl.ds(u * chunks + c, 1), :] = relaxed[
                    k, pl.ds(row, 1), pl.ds(c * 128, 128)
                ]

    def pack_columns(planes, box):
        for i, sign in enumerate((1, -1)):
            lane = width - 128 if sign > 0 else 0
            units = column_units(planes, sign)
            for t in range(0, len(units), GROUPS):
                parts = {}
                for place, (k, n) in enumerate(units[t : t + GROUPS]):
                    own = GROUPS - 1 - n if sign > 0 else n
                    parts.setdefault((k, place - own), []).append(place)
                for top in range(0, rows, 8):
                    box[i, pl.ds(t // GROUPS * rows + top, 8), :] = merge(
                        [
                            (turned(relaxed[k, pl.ds(top, 8), pl.ds(lane, 128)], by), places)
                            for (k, by), places in parts.items()
                        ]
                    )

    def unpack_rows(planes, box):
        for i, sign in enumerate((1, -1)):
            for u, (k, n) in enumerate(row_units(planes, sign)):
                row = tall - 1 - n if sign > 0 else rows + n
                for c in range(chunks):
                    relaxed[k, pl.ds(row, 1), pl.ds(c * 128, 128)] = box[
                        i, pl.ds(u * chunks + c, 1), :
                    ]

    def unpack_columns(planes, box):
        for top in range(0, rows, 8):
            for k in range(planes):
                parts = {}
                for i, sign in enumerate((1, -1)):
                    units = column_units(planes, sign)
                    for n in range(layers_of(k, 1, sign)):
                        u = units.index((k, n))
                        own = GROUPS - 1 - n if sign > 0 else n
                        parts.setdefault((i, u // GROUPS, own - u % GROUPS), []).append(own)
                relaxed[k, pl.ds(top, 8), pl.ds(width, 128)] = merge(
                    [
                        (turned(box[i, pl.ds(t * rows + top, 8), :], by), places)
                        for (i, t, by), places in parts.items()
                    ]
                )

    def unpack_corners(planes, box):
        for i, (sign_x, sign_y) in enumerate(SENDS[4:]):
            height, places = corner_units(planes, sign_x, sign_y)
            for j, units in enumerate(places):
                m = 1 if j == 3 else 0
                own = GROUPS - 1 - m if sign_y > 0 else m
                for top in range(0, len(units), 8):
                    count = min(8, height - top)
                    stage[i, j, pl.ds(top, count), :] = turned(
                        box[i, pl.ds(top, count), :], own - j
                    )
                for u, (k, n, _) in enumerate(units):
                    row = tall - 1 - n if sign_x > 0 else rows + n
                    at = (k, pl.ds(row, 1), pl.ds(width, 128))
                    relaxed[at] = jnp.where(
                        group[:1] == own, stage[i, j, pl.ds(u, 1), :], relaxed[at]
                    )

    height = lax.broadcasted_iota(jnp.int32, (tall, wide), 1) % NZ

    near = lax.broadcasted_iota(jnp.int32, (8, wide), 1) % NZ
    edge = lax.broadcasted_iota(jnp.int32, (8, wide), 0)

    def pass_margin():
        last = pl.ds(rows - 8, 8)
        outer = pl.ds(rows, 8)
        first = pl.ds(0, 8)
        for k in range(POPS):
            step_x, step_y, step_z = MOVES[k]
            by = (step_y * NZ + step_z) % wide

            def along(at, k=k, by=by):
                return pltpu.roll(relaxed[k, at, :], by, 1) if by else relaxed[k, at, :]

            cells = along(outer)
            if step_x > 0:
                turn = pltpu.roll(cells, 1, 0)
                cells = jnp.where(edge == 0, pltpu.roll(along(last), 1, 0), turn)
                take = edge == 0
                if step_z:
                    take = take & (near != (0 if step_z == 1 else NZ - 1))
                state[k, first, :] = jnp.where(take, turn, state[k, first, :])
            elif step_x < 0:
                turn = pltpu.roll(cells, 7, 0)
                cells = jnp.where(edge == 7, pltpu.roll(along(first), 7, 0), turn)
                take = edge == 7
                if step_z:
                    take = take & (near != (0 if step_z == 1 else NZ - 1))
                state[k, last, :] = jnp.where(take, turn, state[k, last, :])
            if step_z:
                cells = jnp.where(
                    near == (0 if step_z == 1 else NZ - 1), relaxed[BACK[k], outer, :], cells
                )
            state[k, outer, :] = cells

    def copies(step):
        x_out, x_got, y_out, y_got, c_out, c_got = boxes[6 * step : 6 * step + 6]
        pairs = []
        for side in range(8):
            if side < 2:
                source, target = x_out.at[side], x_got.at[side]
            elif side < 4:
                source, target = y_out.at[side - 2], y_got.at[side - 2]
            else:
                source, target = c_out.at[side - 4], c_got.at[side - 4]
            pairs.append(
                pltpu.make_async_remote_copy(
                    src_ref=source,
                    dst_ref=target,
                    send_sem=send_sem.at[step, side],
                    recv_sem=recv_sem.at[step, side],
                    device_id=device(side),
                    device_id_type=MESH,
                )
            )
        return pairs

    for step in range(ROUNDS):
        planes = POPS if step else PLANES
        x_out, x_got, y_out, y_got, c_out, c_got = boxes[6 * step : 6 * step + 6]
        sent = copies(step)
        upper = lax.rem(gx, 2)
        last = rows // 8 - 1
        relax_row(upper * last, UNROLL)
        for index in range(1, last):
            relax_row(index, UNROLL)
        if step == 0:
            pl.semaphore_wait(barrier, 8)
        for side in (0, 1):

            @pl.when(upper == 1 - side)
            def _():
                pack_rows(planes, x_out, side)
                sent[side].start()

        relax_row((1 - upper) * last, UNROLL)
        pack_columns(planes, y_out)
        for side in (2, 3):
            sent[side].start()
        pack_corners(planes, c_out)
        for side in range(4, 8):
            sent[side].start()
        for side in (0, 1):

            @pl.when(upper == side)
            def _():
                pack_rows(planes, x_out, side)
                sent[side].start()

        for side in (2, 3):
            sent[side].wait_recv()
        unpack_columns(planes, y_got)
        for k in range(POPS):
            state[k, pl.ds(0, rows), :] = passed(relaxed, k, height)[:rows]
        for side in (4, 5, 6, 7):
            sent[side].wait_recv()
        unpack_corners(planes, c_got)
        for side in (0, 1):
            sent[side].wait_recv()
        unpack_rows(planes, x_got)
        for copy in sent:
            copy.wait_send()
        pass_margin()
        relax(tall // 8, wide // 128, UNROLL_ALL)
        if step < ROUNDS - 1:
            for k in range(POPS):
                state[k, pl.ds(0, rows), pl.ds(0, width)] = passed(relaxed, k, height)[
                    :rows, :width
                ]


def passed(relaxed, k, height):
    step_x, step_y, step_z = MOVES[k]
    tall, wide = height.shape
    cells = relaxed[k]
    by = (step_y * NZ + step_z) % wide
    if by:
        cells = pltpu.roll(cells, by, 1)
    if step_x:
        cells = pltpu.roll(cells, step_x % tall, 0)
    if step_z:
        cells = jnp.where(height == (0 if step_z == 1 else NZ - 1), relaxed[BACK[k]], cells)
    return cells


def finish(relaxed, flow_out, trace_out, flow, trace, out_sem):
    rows, width = flow.shape[1:]
    height = lax.broadcasted_iota(jnp.int32, relaxed.shape[1:], 1) % NZ
    writes = []
    for k in range(POPS):
        near, far, at = (flow, flow_out, k) if k < FLOW else (trace, trace_out, k - FLOW)
        near[at] = passed(relaxed, k, height)[:rows, :width]
        writes.append(pltpu.make_async_copy(near.at[at], far.at[at], out_sem.at[k]))
        if k:
            writes[k - 1].start()
    writes[POPS - 1].start()
    for write in writes:
        write.wait()


def local(sizes, populations, tracer, solid_mask, inflow, wind_profile, emission):
    rows, width = solid_mask.shape
    chunks = width // 128
    tall, wide = rows + ROW_MARGIN, width + LANE_MARGIN
    far = pl.BlockSpec(memory_space=pltpu.HBM)
    near = pl.BlockSpec(memory_space=pltpu.VMEM)
    boxes = []
    for step in range(ROUNDS):
        kind = 1 if step else 0
        for shape in (
            (2, ROWS_OF[kind] * chunks, 128),
            (2, TILES_OF[kind] * rows, 128),
            (4, CORNER_OF[kind], 128),
        ):
            boxes += [pltpu.VMEM(shape, jnp.float32)] * 2
    held_far = [
        pltpu.with_memory_space_constraint(a, pltpu.HBM)
        for a in (populations, tracer, solid_mask, inflow, wind_profile, emission)
    ]
    relaxed = pl.pallas_call(
        functools.partial(exchange, sizes),
        out_shape=pltpu.VMEM((PLANES, tall, wide), jnp.float32),
        in_specs=[far] * 6,
        out_specs=near,
        scratch_shapes=[
            pltpu.VMEM((POPS, tall, wide), jnp.float32),
            pltpu.VMEM((rows, width), jnp.int32),
            pltpu.VMEM((rows, width), jnp.int32),
            pltpu.VMEM(wind_profile.shape, jnp.float32),
            pltpu.VMEM((FLOW, 8, 128), jnp.float32),
            pltpu.VMEM((4, 4, 16, 128), jnp.float32),
            pltpu.SemaphoreType.DMA((6,)),
            pltpu.SemaphoreType.DMA((ROUNDS, 8)),
            pltpu.SemaphoreType.DMA((ROUNDS, 8)),
            *boxes,
        ],
        compiler_params=pltpu.CompilerParams(
            collective_id=0, has_side_effects=True, vmem_limit_bytes=24 << 20
        ),
        name="exchange",
    )(*held_far)
    return pl.pallas_call(
        finish,
        out_shape=(
            jax.ShapeDtypeStruct(populations.shape, jnp.float32),
            jax.ShapeDtypeStruct(tracer.shape, jnp.float32),
        ),
        in_specs=[near],
        out_specs=(far, far),
        scratch_shapes=[
            pltpu.VMEM(populations.shape, jnp.float32),
            pltpu.VMEM(tracer.shape, jnp.float32),
            pltpu.SemaphoreType.DMA((POPS,)),
        ],
        compiler_params=pltpu.CompilerParams(vmem_limit_bytes=16 << 20),
        name="finish",
    )(pltpu.with_memory_space_constraint(relaxed, pltpu.VMEM))


def solution(mesh):
    sizes = (mesh.shape["gx"], mesh.shape["gy"])
    in_specs = (
        P(None, "gx", "gy"),
        P(None, "gx", "gy"),
        P("gx", "gy"),
        P("gx", "gy"),
        P(),
        P("gx", "gy"),
    )
    out_specs = (P(None, "gx", "gy"), P(None, "gx", "gy"))
    return jax.shard_map(
        functools.partial(local, sizes),
        mesh=mesh,
        in_specs=in_specs,
        out_specs=out_specs,
        check_vma=False,
    )
```

```python
import functools
import math

import jax
import jax.numpy as jnp
from jax import lax
from jax.experimental import pallas as pl
from jax.experimental.pallas import tpu as pltpu
from jax.sharding import PartitionSpec as P

NZ = 32
STEPS = 4
FLOW = 19
TRACE = 7
POPS = FLOW + TRACE

LATTICE = (
    (0, 0, 0),
    (1, 0, 0),
    (-1, 0, 0),
    (0, 1, 0),
    (0, -1, 0),
    (0, 0, 1),
    (0, 0, -1),
    (1, 1, 0),
    (-1, -1, 0),
    (1, -1, 0),
    (-1, 1, 0),
    (1, 0, 1),
    (-1, 0, -1),
    (1, 0, -1),
    (-1, 0, 1),
    (0, 1, 1),
    (0, -1, -1),
    (0, 1, -1),
    (0, -1, 1),
)
OPPOSITE = (0, 2, 1, 4, 3, 6, 5, 8, 7, 10, 9, 12, 11, 14, 13, 16, 15, 18, 17)
MOVES = LATTICE + LATTICE[:TRACE]
BACK = OPPOSITE + tuple(FLOW + k for k in OPPOSITE[:TRACE])
BASE_RELAX = 0.6
SMAGORINSKY = 0.2
TRACER_RELAX = 0.7

PLANES = POPS + 3
DEPTH = 2
ROUNDS = STEPS // DEPTH
SENDS = ((1, 0), (-1, 0), (0, 1), (0, -1), (1, 1), (-1, -1), (1, -1), (-1, 1))
MESH = pl.DeviceIdType.MESH
GROUPS = 128 // NZ
UNROLL = 2
UNROLL_ALL = 3
ROW_MARGIN = 8
LANE_MARGIN = 128


def layers_of(k, axis, sign):
    if k >= POPS:
        return DEPTH - 1
    toward = MOVES[k][axis] * sign
    if toward > 0:
        return DEPTH
    if toward == 0:
        return DEPTH - 1
    return DEPTH - 1 if MOVES[k][2] != 0 else DEPTH - 2


def row_units(planes, sign):
    return [(k, n) for k in range(planes) for n in range(layers_of(k, 0, sign))]


def column_units(planes, sign):
    pairs = [k for k in range(planes) if layers_of(k, 1, sign) == DEPTH]
    singles = [k for k in range(planes) if layers_of(k, 1, sign) == DEPTH - 1]
    return [(k, n) for k in pairs for n in range(DEPTH)] + [(k, 0) for k in singles]


def corner_units(planes, sign_x, sign_y):
    units = [
        (k, n, m)
        for k in range(planes)
        for n in range(layers_of(k, 0, sign_x))
        for m in range(layers_of(k, 1, sign_y))
    ]
    near = [u for u in units if u[2] == 0]
    far = [u for u in units if u[2] == 1]
    height = -(-len(near) // 3)
    return height, [near[:height], near[height : 2 * height], near[2 * height :], far]


ROWS_OF = [len(row_units(p, 1)) for p in (PLANES, POPS)]
TILES_OF = [-(-len(column_units(p, 1)) // GROUPS) for p in (PLANES, POPS)]
CORNER_OF = [corner_units(p, 1, 1)[0] for p in (PLANES, POPS)]


def inflow_states(wind):
    square = wind[0] * wind[0] + wind[1] * wind[1] + wind[2] * wind[2]
    held = []
    for k in range(FLOW):
        along = sum(LATTICE[k][a] * wind[a] for a in range(3) if LATTICE[k][a] != 0)
        held.append(1.0 + 3.0 * along + 4.5 * along * along - 1.5 * square)
    return held


def relax_cells(h, q, solid, inflow, emission, held):
    total = {k: h[k] + h[k + 1] for k in range(1, FLOW, 2)}
    delta = {k: h[k] - h[k + 1] for k in range(1, FLOW, 2)}
    in_xy, in_xz, in_yz = total[7] + total[9], total[11] + total[13], total[15] + total[17]
    twice = [total[k] + total[k] for k in (1, 3, 5)]
    moment = [twice[0] + (in_xy + in_xz), twice[1] + (in_xy + in_yz), twice[2] + (in_xz + in_yz)]
    density = (12.0 * h[0] + moment[0]) + ((twice[1] + twice[2]) + in_yz)
    drive = [
        (delta[1] + delta[1]) + ((delta[7] + delta[9]) + (delta[11] + delta[13])),
        (delta[3] + delta[3]) + ((delta[7] - delta[9]) + (delta[15] + delta[17])),
        (delta[5] + delta[5]) + ((delta[11] - delta[13]) + (delta[15] - delta[17])),
    ]
    speed = [d * (1.0 / 6.0) for d in drive]
    square = [v * v for v in speed]
    cross = [speed[0] * speed[1], speed[0] * speed[2], speed[1] * speed[2]]
    third = density * (1.0 / 3.0)
    stress = [(moment[a] - third) - square[a] for a in range(3)]
    shear = [
        (total[7] - total[9]) - cross[0],
        (total[11] - total[13]) - cross[1],
        (total[15] - total[17]) - cross[2],
    ]
    sheared = (shear[0] * shear[0] + shear[1] * shear[1]) + shear[2] * shear[2]
    contraction = ((stress[0] * stress[0] + stress[1] * stress[1]) + stress[2] * stress[2]) + (
        sheared + sheared
    )
    gain = 18.0 * math.sqrt(2.0) * SMAGORINSKY * SMAGORINSKY / 36.0
    inner = BASE_RELAX * BASE_RELAX + gain * jnp.sqrt(contraction)
    half = 1.0 / (BASE_RELAX + inner * lax.rsqrt(inner))
    keep = 1.0 - (half + half)
    base = half * (
        density * (1.0 / 18.0) - ((square[0] + square[1]) + square[2]) * (1.0 / 12.0)
    )
    lean = [half * v for v in speed]
    quarter = 0.25 * half
    bend = [quarter * v for v in square]
    twist = [(0.5 * half) * v for v in cross]
    straight = [base + v for v in bend]
    slant = [straight[0] + bend[1], straight[0] + bend[2], straight[1] + bend[2]]

    def settle(k, fluid):
        return jnp.where(solid, h[OPPOSITE[k]], jnp.where(inflow, held(k), fluid))

    relaxed = [settle(0, keep * h[0] + base)]

    def pair(k, even, odd):
        relaxed.append(settle(k, keep * h[k] + (even + odd)))
        relaxed.append(settle(k + 1, keep * h[k + 1] + (even - odd)))

    for a in range(3):
        pair(2 * a + 1, straight[a], lean[a])
    for i, (a, b) in enumerate(((0, 1), (0, 2), (1, 2))):
        pair(4 * i + 7, slant[i] + twist[i], lean[a] + lean[b])
        pair(4 * i + 9, slant[i] - twist[i], lean[a] - lean[b])

    share = (0.25 / TRACER_RELAX) * q[0] + (0.125 / TRACER_RELAX) * (
        (q[1] + q[2]) + (q[3] + q[4]) + (q[5] + q[6])
    )
    level = share + emission
    drift = share * (2.0 / 3.0)
    rest = 1.0 - 1.0 / TRACER_RELAX

    def trace(k, fluid):
        return jnp.where(solid, q[OPPOSITE[k]], jnp.where(inflow, 0.0, fluid))

    traced = [trace(0, rest * q[0] + level)]
    for k in range(1, TRACE, 2):
        carried = drift * speed[(k - 1) // 2]
        traced.append(trace(k, rest * q[k] + (level + carried)))
        traced.append(trace(k + 1, rest * q[k + 1] + (level - carried)))
    return relaxed, traced


def exchange(
    sizes,
    flow_in,
    trace_in,
    solid_in,
    inflow_in,
    wind_in,
    emission_in,
    relaxed,
    state,
    solid,
    inflow,
    wind,
    held,
    stage,
    in_sem,
    send_sem,
    recv_sem,
    passing,
    pass_sem,
    *boxes,
):
    rows, width = solid.shape
    chunks = width // 128
    tall, wide = rows + ROW_MARGIN, width + LANE_MARGIN
    gx, gy = lax.axis_index("gx"), lax.axis_index("gy")

    def device(side):
        step_x, step_y = SENDS[side]
        return (
            lax.rem(gx + step_x + sizes[0], sizes[0]),
            lax.rem(gy + step_y + sizes[1], sizes[1]),
        )

    upper = lax.rem(gx, 2)
    plane = lax.rem(gx // 2, 2) * 4 + lax.rem(gy, 4)
    first_out = [
        jnp.logical_not((plane == 0) & (upper == {6: 1, 5: 0}[side]))
        if side in (5, 6)
        else None
        for side in range(8)
    ]

    barrier = pltpu.get_barrier_semaphore()

    def greet(side):
        pl.semaphore_signal(barrier, inc=1, device_id=device(side), device_id_type=MESH)

    for side in range(8):
        if side in (4, 7):

            @pl.when(jnp.logical_not((plane == 7) & (upper == {4: 1, 7: 0}[side])))
            def _():
                greet(side)

        else:
            greet(side)

    block = (slice(None), pl.ds(0, rows), pl.ds(0, width))
    loads = [
        pltpu.make_async_copy(source, target, in_sem.at[i])
        for i, (source, target) in enumerate(
            (
                (flow_in, state.at[pl.ds(0, FLOW), pl.ds(0, rows), pl.ds(0, width)]),
                (trace_in, state.at[pl.ds(FLOW, TRACE), pl.ds(0, rows), pl.ds(0, width)]),
                (solid_in, solid),
                (inflow_in, inflow),
                (emission_in, relaxed.at[PLANES - 1, pl.ds(0, rows), pl.ds(0, width)]),
                (wind_in, wind),
            )
        )
    ]
    for load in loads:
        load.start()
    for load in loads:
        load.wait()
    winds = [jnp.concatenate([wind[a : a + 1, :]] * GROUPS, axis=1) for a in range(3)]
    for k, cells in enumerate(inflow_states(winds)):
        held[k] = jnp.broadcast_to(cells, (8, 128))
    relaxed[POPS, pl.ds(0, rows), pl.ds(0, width)] = jnp.where(solid[...] == 1, 1.0, 0.0)
    relaxed[POPS + 1, pl.ds(0, rows), pl.ds(0, width)] = jnp.where(inflow[...] == 1, 1.0, 0.0)

    def relax_tile(row_tile, lane_tile):
        row = pl.ds(pl.multiple_of(row_tile * 8, 8), 8)
        lane = pl.ds(pl.multiple_of(lane_tile * 128, 128), 128)
        settled, traced = relax_cells(
            [state[k, row, lane] for k in range(FLOW)],
            [state[FLOW + k, row, lane] for k in range(TRACE)],
            relaxed[POPS, row, lane] == 1.0,
            relaxed[POPS + 1, row, lane] == 1.0,
            relaxed[POPS + 2, row, lane],
            lambda k: held[k],
        )
        for k, cells in enumerate(settled + traced):
            relaxed[k, row, lane] = cells

    def relax(row_tiles, lane_tiles, unroll):
        def tiles(index, carry):
            for i in range(unroll):
                at = index * unroll + i
                relax_tile(at // lane_tiles, at % lane_tiles)
            return carry

        lax.fori_loop(0, row_tiles * lane_tiles // unroll, tiles, 0)

    def relax_row(row_tile, unroll):
        def tiles(index, carry):
            for i in range(unroll):
                relax_tile(row_tile, index * unroll + i)
            return carry

        lax.fori_loop(0, chunks // unroll, tiles, 0)

    group = lax.broadcasted_iota(jnp.int32, (8, 128), 1) // NZ

    def merge(pieces):
        cells = pieces[0][0]
        for piece, places in pieces[1:]:
            take = functools.reduce(jnp.logical_or, [group == p for p in places])
            cells = jnp.where(take, piece, cells)
        return cells

    def turned(piece, by):
        by = by * NZ % 128
        return pltpu.roll(piece, by, 1) if by else piece

    def pack_corner(planes, box, i, side, row_of):
        sign_x, sign_y = SENDS[side]
        lane = width - 128 if sign_y > 0 else 0
        height, places = corner_units(planes, sign_x, sign_y)
        for j, units in enumerate(places):
            for u, (k, n, m) in enumerate(units):
                stage[i, j, pl.ds(u, 1), :] = relaxed[k, pl.ds(row_of(n), 1), pl.ds(lane, 128)]
        for top in range(0, height, 8):
            pieces = []
            for j in range(4):
                m = 1 if j == 3 else 0
                own = GROUPS - 1 - m if sign_y > 0 else m
                pieces.append((turned(stage[i, j, pl.ds(top, 8), :], j - own), [j]))
            count = min(8, height - top)
            box[i, pl.ds(top, count), :] = merge(pieces)[:count]

    def pack_corners(planes, box):
        for i, (sign_x, _) in enumerate(SENDS[4:]):
            pack_corner(
                planes, box, i, 4 + i, (lambda n: rows - 1 - n) if sign_x > 0 else (lambda n: n)
            )

    def pack_rows(planes, box, i):
        sign = SENDS[i][0]
        for u, (k, n) in enumerate(row_units(planes, sign)):
            row = rows - 1 - n if sign > 0 else n
            for c in range(chunks):
                box[i, pl.ds(u * chunks + c, 1), :] = relaxed[
                    k, pl.ds(row, 1), pl.ds(c * 128, 128)
                ]

    def pack_columns(planes, box):
        for i, sign in enumerate((1, -1)):
            lane = width - 128 if sign > 0 else 0
            units = column_units(planes, sign)
            for t in range(0, len(units), GROUPS):
                parts = {}
                for place, (k, n) in enumerate(units[t : t + GROUPS]):
                    own = GROUPS - 1 - n if sign > 0 else n
                    parts.setdefault((k, place - own), []).append(place)
                for top in range(0, rows, 8):
                    box[i, pl.ds(t // GROUPS * rows + top, 8), :] = merge(
                        [
                            (turned(relaxed[k, pl.ds(top, 8), pl.ds(lane, 128)], by), places)
                            for (k, by), places in parts.items()
                        ]
                    )

    def unpack_rows(planes, box, i):
        sign = SENDS[i][0]
        for u, (k, n) in enumerate(row_units(planes, sign)):
            row = tall - 1 - n if sign > 0 else rows + n
            for c in range(chunks):
                relaxed[k, pl.ds(row, 1), pl.ds(c * 128, 128)] = box[
                    i, pl.ds(u * chunks + c, 1), :
                ]

    def unpack_columns(planes, box):
        for top in range(0, rows, 8):
            for k in range(planes):
                parts = {}
                for i, sign in enumerate((1, -1)):
                    units = column_units(planes, sign)
                    for n in range(layers_of(k, 1, sign)):
                        u = units.index((k, n))
                        own = GROUPS - 1 - n if sign > 0 else n
                        parts.setdefault((i, u // GROUPS, own - u % GROUPS), []).append(own)
                relaxed[k, pl.ds(top, 8), pl.ds(width, 128)] = merge(
                    [
                        (turned(box[i, pl.ds(t * rows + top, 8), :], by), places)
                        for (i, t, by), places in parts.items()
                    ]
                )

    def unpack_corners(planes, box):
        for i, (sign_x, sign_y) in enumerate(SENDS[4:]):
            height, places = corner_units(planes, sign_x, sign_y)
            for j, units in enumerate(places):
                m = 1 if j == 3 else 0
                own = GROUPS - 1 - m if sign_y > 0 else m
                for top in range(0, len(units), 8):
                    count = min(8, height - top)
                    stage[i, j, pl.ds(top, count), :] = turned(
                        box[i, pl.ds(top, count), :], own - j
                    )
                for u, (k, n, _) in enumerate(units):
                    row = tall - 1 - n if sign_x > 0 else rows + n
                    at = (k, pl.ds(row, 1), pl.ds(width, 128))
                    relaxed[at] = jnp.where(
                        group[:1] == own, stage[i, j, pl.ds(u, 1), :], relaxed[at]
                    )

    height = lax.broadcasted_iota(jnp.int32, (tall, wide), 1) % NZ

    near = lax.broadcasted_iota(jnp.int32, (8, wide), 1) % NZ
    edge = lax.broadcasted_iota(jnp.int32, (8, wide), 0)

    def pass_margin():
        last = pl.ds(rows - 8, 8)
        outer = pl.ds(rows, 8)
        first = pl.ds(0, 8)
        for k in range(POPS):
            step_x, step_y, step_z = MOVES[k]
            by = (step_y * NZ + step_z) % wide

            def along(at, k=k, by=by):
                return pltpu.roll(relaxed[k, at, :], by, 1) if by else relaxed[k, at, :]

            cells = along(outer)
            if step_x > 0:
                turn = pltpu.roll(cells, 1, 0)
                cells = jnp.where(edge == 0, pltpu.roll(along(last), 1, 0), turn)
                take = edge == 0
                if step_z:
                    take = take & (near != (0 if step_z == 1 else NZ - 1))
                state[k, first, :] = jnp.where(take, turn, state[k, first, :])
            elif step_x < 0:
                turn = pltpu.roll(cells, 7, 0)
                cells = jnp.where(edge == 7, pltpu.roll(along(first), 7, 0), turn)
                take = edge == 7
                if step_z:
                    take = take & (near != (0 if step_z == 1 else NZ - 1))
                state[k, last, :] = jnp.where(take, turn, state[k, last, :])
            if step_z:
                cells = jnp.where(
                    near == (0 if step_z == 1 else NZ - 1), relaxed[BACK[k], outer, :], cells
                )
            state[k, outer, :] = cells

    def carry_on(side):
        return pltpu.make_async_remote_copy(
            src_ref=passing.at[0],
            dst_ref=boxes[5].at[side - 4],
            send_sem=pass_sem,
            recv_sem=recv_sem.at[0, side],
            device_id=device(3),
            device_id_type=MESH,
        )

    def copies(step):
        x_out, x_got, y_out, y_got, c_out, c_got = boxes[6 * step : 6 * step + 6]
        pairs = []
        for side in range(8):
            if side < 2:
                source, target = x_out.at[side], x_got.at[side]
            elif side < 4:
                source, target = y_out.at[side - 2], y_got.at[side - 2]
            else:
                source, target = c_out.at[side - 4], c_got.at[side - 4]
            pairs.append(
                pltpu.make_async_remote_copy(
                    src_ref=source,
                    dst_ref=target,
                    send_sem=send_sem.at[step, side],
                    recv_sem=recv_sem.at[step, side],
                    device_id=device(side),
                    device_id_type=MESH,
                )
            )
        return pairs

    for step in range(ROUNDS):
        planes = POPS if step else PLANES
        x_out, x_got, y_out, y_got, c_out, c_got = boxes[6 * step : 6 * step + 6]
        sent = copies(step)
        last = rows // 8 - 1
        relax_row(upper * last, UNROLL)
        for index in range(1, last):
            relax_row(index, UNROLL)
        if step == 0:
            pl.semaphore_wait(barrier, jnp.where(plane == 0, 7, 8))
        for side in (0, 1):

            @pl.when(upper == 1 - side)
            def _():
                pack_rows(planes, x_out, side)
                sent[side].start()

        relax_row((1 - upper) * last, UNROLL)
        pack_columns(planes, y_out)
        for side in (2, 3):
            sent[side].start()
        pack_corners(planes, c_out)
        for side in range(4, 8):
            if step == 0 and first_out[side] is not None:
                pl.when(first_out[side])(sent[side].start)
            else:
                sent[side].start()
        for side in (0, 1):

            @pl.when(upper == side)
            def _():
                pack_rows(planes, x_out, side)
                sent[side].start()

        if step == 0:
            for side in (0, 1):

                @pl.when((plane == 4) & (upper == side))
                def _():
                    sent[side].wait_recv()
                    unpack_rows(planes, x_got, side)
                    onward = 6 - side
                    pack_corner(
                        planes,
                        passing,
                        0,
                        onward,
                        (lambda n: tall - 1 - n) if side == 0 else (lambda n: rows + n),
                    )
                    carry_on(onward).start()

        for side in (2, 3):
            sent[side].wait_recv()
        unpack_columns(planes, y_got)
        for k in range(POPS):
            state[k, pl.ds(0, rows), :] = passed(relaxed, k, height)[:rows]
        for side in (4, 5, 6, 7):
            sent[side].wait_recv()
        unpack_corners(planes, c_got)
        for side in (0, 1):

            def take_rows(side=side):
                sent[side].wait_recv()
                unpack_rows(planes, x_got, side)

            if step == 0:
                pl.when(jnp.logical_not((plane == 4) & (upper == side)))(take_rows)
            else:
                take_rows()
        for side in range(8):
            if step == 0 and first_out[side] is not None:
                pl.when(first_out[side])(sent[side].wait_send)
            else:
                sent[side].wait_send()
        if step == 0:
            for side in (0, 1):

                @pl.when((plane == 4) & (upper == side))
                def _():
                    carry_on(6 - side).wait_send()

        pass_margin()
        relax(tall // 8, wide // 128, UNROLL_ALL)
        if step < ROUNDS - 1:
            for k in range(POPS):
                state[k, pl.ds(0, rows), pl.ds(0, width)] = passed(relaxed, k, height)[
                    :rows, :width
                ]


def passed(relaxed, k, height):
    step_x, step_y, step_z = MOVES[k]
    tall, wide = height.shape
    cells = relaxed[k]
    by = (step_y * NZ + step_z) % wide
    if by:
        cells = pltpu.roll(cells, by, 1)
    if step_x:
        cells = pltpu.roll(cells, step_x % tall, 0)
    if step_z:
        cells = jnp.where(height == (0 if step_z == 1 else NZ - 1), relaxed[BACK[k]], cells)
    return cells


def finish(relaxed, flow_out, trace_out, flow, trace, out_sem):
    rows, width = flow.shape[1:]
    height = lax.broadcasted_iota(jnp.int32, relaxed.shape[1:], 1) % NZ
    writes = []
    for k in range(POPS):
        near, far, at = (flow, flow_out, k) if k < FLOW else (trace, trace_out, k - FLOW)
        near[at] = passed(relaxed, k, height)[:rows, :width]
        writes.append(pltpu.make_async_copy(near.at[at], far.at[at], out_sem.at[k]))
        if k:
            writes[k - 1].start()
    writes[POPS - 1].start()
    for write in writes:
        write.wait()


def local(sizes, populations, tracer, solid_mask, inflow, wind_profile, emission):
    rows, width = solid_mask.shape
    chunks = width // 128
    tall, wide = rows + ROW_MARGIN, width + LANE_MARGIN
    far = pl.BlockSpec(memory_space=pltpu.HBM)
    near = pl.BlockSpec(memory_space=pltpu.VMEM)
    boxes = []
    for step in range(ROUNDS):
        kind = 1 if step else 0
        for shape in (
            (2, ROWS_OF[kind] * chunks, 128),
            (2, TILES_OF[kind] * rows, 128),
            (4, CORNER_OF[kind], 128),
        ):
            boxes += [pltpu.VMEM(shape, jnp.float32)] * 2
    held_far = [
        pltpu.with_memory_space_constraint(a, pltpu.HBM)
        for a in (populations, tracer, solid_mask, inflow, wind_profile, emission)
    ]
    relaxed = pl.pallas_call(
        functools.partial(exchange, sizes),
        out_shape=pltpu.VMEM((PLANES, tall, wide), jnp.float32),
        in_specs=[far] * 6,
        out_specs=near,
        scratch_shapes=[
            pltpu.VMEM((POPS, tall, wide), jnp.float32),
            pltpu.VMEM((rows, width), jnp.int32),
            pltpu.VMEM((rows, width), jnp.int32),
            pltpu.VMEM(wind_profile.shape, jnp.float32),
            pltpu.VMEM((FLOW, 8, 128), jnp.float32),
            pltpu.VMEM((4, 4, 16, 128), jnp.float32),
            pltpu.SemaphoreType.DMA((6,)),
            pltpu.SemaphoreType.DMA((ROUNDS, 8)),
            pltpu.SemaphoreType.DMA((ROUNDS, 8)),
            pltpu.VMEM((1, CORNER_OF[0], 128), jnp.float32),
            pltpu.SemaphoreType.DMA,
            *boxes,
        ],
        compiler_params=pltpu.CompilerParams(
            collective_id=0, has_side_effects=True, vmem_limit_bytes=24 << 20
        ),
        name="exchange",
    )(*held_far)
    return pl.pallas_call(
        finish,
        out_shape=(
            jax.ShapeDtypeStruct(populations.shape, jnp.float32),
            jax.ShapeDtypeStruct(tracer.shape, jnp.float32),
        ),
        in_specs=[near],
        out_specs=(far, far),
        scratch_shapes=[
            pltpu.VMEM(populations.shape, jnp.float32),
            pltpu.VMEM(tracer.shape, jnp.float32),
            pltpu.SemaphoreType.DMA((POPS,)),
        ],
        compiler_params=pltpu.CompilerParams(vmem_limit_bytes=16 << 20),
        name="finish",
    )(pltpu.with_memory_space_constraint(relaxed, pltpu.VMEM))


def solution(mesh):
    sizes = (mesh.shape["gx"], mesh.shape["gy"])
    in_specs = (
        P(None, "gx", "gy"),
        P(None, "gx", "gy"),
        P("gx", "gy"),
        P("gx", "gy"),
        P(),
        P("gx", "gy"),
    )
    out_specs = (P(None, "gx", "gy"), P(None, "gx", "gy"))
    return jax.shard_map(
        functools.partial(local, sizes),
        mesh=mesh,
        in_specs=in_specs,
        out_specs=out_specs,
        check_vma=False,
    )
```

```python
import functools
import math

import jax
import jax.numpy as jnp
from jax import lax
from jax.experimental import pallas as pl
from jax.experimental.pallas import tpu as pltpu
from jax.sharding import PartitionSpec as P

NZ = 32
STEPS = 4
FLOW = 19
TRACE = 7
POPS = FLOW + TRACE

LATTICE = (
    (0, 0, 0),
    (1, 0, 0),
    (-1, 0, 0),
    (0, 1, 0),
    (0, -1, 0),
    (0, 0, 1),
    (0, 0, -1),
    (1, 1, 0),
    (-1, -1, 0),
    (1, -1, 0),
    (-1, 1, 0),
    (1, 0, 1),
    (-1, 0, -1),
    (1, 0, -1),
    (-1, 0, 1),
    (0, 1, 1),
    (0, -1, -1),
    (0, 1, -1),
    (0, -1, 1),
)
OPPOSITE = (0, 2, 1, 4, 3, 6, 5, 8, 7, 10, 9, 12, 11, 14, 13, 16, 15, 18, 17)
MOVES = LATTICE + LATTICE[:TRACE]
BACK = OPPOSITE + tuple(FLOW + k for k in OPPOSITE[:TRACE])
BASE_RELAX = 0.6
SMAGORINSKY = 0.2
TRACER_RELAX = 0.7

PLANES = POPS + 3
DEPTH = 2
ROUNDS = STEPS // DEPTH
SENDS = ((1, 0), (-1, 0), (0, 1), (0, -1), (1, 1), (-1, -1), (1, -1), (-1, 1))
MESH = pl.DeviceIdType.MESH
GROUPS = 128 // NZ
UNROLL = 2
UNROLL_ALL = 3
ROW_MARGIN = 8
LANE_MARGIN = 128


def layers_of(k, axis, sign):
    if k >= POPS:
        return DEPTH - 1
    toward = MOVES[k][axis] * sign
    if toward > 0:
        return DEPTH
    if toward == 0:
        return DEPTH - 1
    return DEPTH - 1 if MOVES[k][2] != 0 else DEPTH - 2


def row_units(planes, sign):
    return [(k, n) for k in range(planes) for n in range(layers_of(k, 0, sign))]


def column_units(planes, sign):
    pairs = [k for k in range(planes) if layers_of(k, 1, sign) == DEPTH]
    singles = [k for k in range(planes) if layers_of(k, 1, sign) == DEPTH - 1]
    return [(k, n) for k in pairs for n in range(DEPTH)] + [(k, 0) for k in singles]


def corner_units(planes, sign_x, sign_y):
    units = [
        (k, n, m)
        for k in range(planes)
        for n in range(layers_of(k, 0, sign_x))
        for m in range(layers_of(k, 1, sign_y))
    ]
    near = [u for u in units if u[2] == 0]
    far = [u for u in units if u[2] == 1]
    height = -(-len(near) // 3)
    return height, [near[:height], near[height : 2 * height], near[2 * height :], far]


ROWS_OF = [len(row_units(p, 1)) for p in (PLANES, POPS)]
TILES_OF = [-(-len(column_units(p, 1)) // GROUPS) for p in (PLANES, POPS)]
CORNER_OF = [corner_units(p, 1, 1)[0] for p in (PLANES, POPS)]


def inflow_states(wind):
    square = wind[0] * wind[0] + wind[1] * wind[1] + wind[2] * wind[2]
    held = []
    for k in range(FLOW):
        along = sum(LATTICE[k][a] * wind[a] for a in range(3) if LATTICE[k][a] != 0)
        held.append(1.0 + 3.0 * along + 4.5 * along * along - 1.5 * square)
    return held


def relax_cells(h, q, solid, inflow, emission, held):
    total = {k: h[k] + h[k + 1] for k in range(1, FLOW, 2)}
    delta = {k: h[k] - h[k + 1] for k in range(1, FLOW, 2)}
    in_xy, in_xz, in_yz = total[7] + total[9], total[11] + total[13], total[15] + total[17]
    twice = [total[k] + total[k] for k in (1, 3, 5)]
    moment = [twice[0] + (in_xy + in_xz), twice[1] + (in_xy + in_yz), twice[2] + (in_xz + in_yz)]
    density = (12.0 * h[0] + moment[0]) + ((twice[1] + twice[2]) + in_yz)
    drive = [
        (delta[1] + delta[1]) + ((delta[7] + delta[9]) + (delta[11] + delta[13])),
        (delta[3] + delta[3]) + ((delta[7] - delta[9]) + (delta[15] + delta[17])),
        (delta[5] + delta[5]) + ((delta[11] - delta[13]) + (delta[15] - delta[17])),
    ]
    speed = [d * (1.0 / 6.0) for d in drive]
    square = [v * v for v in speed]
    cross = [speed[0] * speed[1], speed[0] * speed[2], speed[1] * speed[2]]
    third = density * (1.0 / 3.0)
    stress = [(moment[a] - third) - square[a] for a in range(3)]
    shear = [
        (total[7] - total[9]) - cross[0],
        (total[11] - total[13]) - cross[1],
        (total[15] - total[17]) - cross[2],
    ]
    sheared = (shear[0] * shear[0] + shear[1] * shear[1]) + shear[2] * shear[2]
    contraction = ((stress[0] * stress[0] + stress[1] * stress[1]) + stress[2] * stress[2]) + (
        sheared + sheared
    )
    gain = 18.0 * math.sqrt(2.0) * SMAGORINSKY * SMAGORINSKY / 36.0
    inner = BASE_RELAX * BASE_RELAX + gain * jnp.sqrt(contraction)
    half = 1.0 / (BASE_RELAX + inner * lax.rsqrt(inner))
    keep = 1.0 - (half + half)
    base = half * (
        density * (1.0 / 18.0) - ((square[0] + square[1]) + square[2]) * (1.0 / 12.0)
    )
    lean = [half * v for v in speed]
    quarter = 0.25 * half
    bend = [quarter * v for v in square]
    twist = [(0.5 * half) * v for v in cross]
    straight = [base + v for v in bend]
    slant = [straight[0] + bend[1], straight[0] + bend[2], straight[1] + bend[2]]

    def settle(k, fluid):
        return jnp.where(solid, h[OPPOSITE[k]], jnp.where(inflow, held(k), fluid))

    relaxed = [settle(0, keep * h[0] + base)]

    def pair(k, even, odd):
        relaxed.append(settle(k, keep * h[k] + (even + odd)))
        relaxed.append(settle(k + 1, keep * h[k + 1] + (even - odd)))

    for a in range(3):
        pair(2 * a + 1, straight[a], lean[a])
    for i, (a, b) in enumerate(((0, 1), (0, 2), (1, 2))):
        pair(4 * i + 7, slant[i] + twist[i], lean[a] + lean[b])
        pair(4 * i + 9, slant[i] - twist[i], lean[a] - lean[b])

    share = (0.25 / TRACER_RELAX) * q[0] + (0.125 / TRACER_RELAX) * (
        (q[1] + q[2]) + (q[3] + q[4]) + (q[5] + q[6])
    )
    level = share + emission
    drift = share * (2.0 / 3.0)
    rest = 1.0 - 1.0 / TRACER_RELAX

    def trace(k, fluid):
        return jnp.where(solid, q[OPPOSITE[k]], jnp.where(inflow, 0.0, fluid))

    traced = [trace(0, rest * q[0] + level)]
    for k in range(1, TRACE, 2):
        carried = drift * speed[(k - 1) // 2]
        traced.append(trace(k, rest * q[k] + (level + carried)))
        traced.append(trace(k + 1, rest * q[k + 1] + (level - carried)))
    return relaxed, traced


def exchange(
    sizes,
    flow_in,
    trace_in,
    solid_in,
    inflow_in,
    wind_in,
    emission_in,
    relaxed,
    state,
    solid,
    inflow,
    wind,
    held,
    stage,
    in_sem,
    send_sem,
    recv_sem,
    passing,
    pass_sem,
    *boxes,
):
    rows, width = solid.shape
    chunks = width // 128
    tall, wide = rows + ROW_MARGIN, width + LANE_MARGIN
    gx, gy = lax.axis_index("gx"), lax.axis_index("gy")

    def device(side):
        step_x, step_y = SENDS[side]
        return (
            lax.rem(gx + step_x + sizes[0], sizes[0]),
            lax.rem(gy + step_y + sizes[1], sizes[1]),
        )

    upper = lax.rem(gx, 2)
    plane = lax.rem(gx // 2, 2) * 4 + lax.rem(gy, 4)
    first_out = [
        jnp.logical_not((plane == 0) & (upper == {6: 1, 5: 0}[side]))
        if side in (5, 6)
        else None
        for side in range(8)
    ]

    barrier = pltpu.get_barrier_semaphore()

    def greet(side):
        pl.semaphore_signal(barrier, inc=1, device_id=device(side), device_id_type=MESH)

    for side in range(8):
        if side in (4, 7):

            @pl.when(jnp.logical_not((plane == 7) & (upper == {4: 1, 7: 0}[side])))
            def _():
                greet(side)

        else:
            greet(side)

    block = (slice(None), pl.ds(0, rows), pl.ds(0, width))
    loads = [
        pltpu.make_async_copy(source, target, in_sem.at[i])
        for i, (source, target) in enumerate(
            (
                (flow_in, state.at[pl.ds(0, FLOW), pl.ds(0, rows), pl.ds(0, width)]),
                (trace_in, state.at[pl.ds(FLOW, TRACE), pl.ds(0, rows), pl.ds(0, width)]),
                (solid_in, solid),
                (inflow_in, inflow),
                (emission_in, relaxed.at[PLANES - 1, pl.ds(0, rows), pl.ds(0, width)]),
                (wind_in, wind),
            )
        )
    ]
    for load in loads:
        load.start()
    for load in loads:
        load.wait()
    winds = [jnp.concatenate([wind[a : a + 1, :]] * GROUPS, axis=1) for a in range(3)]
    for k, cells in enumerate(inflow_states(winds)):
        held[k] = jnp.broadcast_to(cells, (8, 128))
    relaxed[POPS, pl.ds(0, rows), pl.ds(0, width)] = jnp.where(solid[...] == 1, 1.0, 0.0)
    relaxed[POPS + 1, pl.ds(0, rows), pl.ds(0, width)] = jnp.where(inflow[...] == 1, 1.0, 0.0)

    def relax_tile(row_tile, lane_tile):
        row = pl.ds(pl.multiple_of(row_tile * 8, 8), 8)
        lane = pl.ds(pl.multiple_of(lane_tile * 128, 128), 128)
        settled, traced = relax_cells(
            [state[k, row, lane] for k in range(FLOW)],
            [state[FLOW + k, row, lane] for k in range(TRACE)],
            relaxed[POPS, row, lane] == 1.0,
            relaxed[POPS + 1, row, lane] == 1.0,
            relaxed[POPS + 2, row, lane],
            lambda k: held[k],
        )
        for k, cells in enumerate(settled + traced):
            relaxed[k, row, lane] = cells

    def relax(row_tiles, lane_tiles, unroll):
        def tiles(index, carry):
            for i in range(unroll):
                at = index * unroll + i
                relax_tile(at // lane_tiles, at % lane_tiles)
            return carry

        lax.fori_loop(0, row_tiles * lane_tiles // unroll, tiles, 0)

    def relax_row(row_tile, unroll):
        def tiles(index, carry):
            for i in range(unroll):
                relax_tile(row_tile, index * unroll + i)
            return carry

        lax.fori_loop(0, chunks // unroll, tiles, 0)

    group = lax.broadcasted_iota(jnp.int32, (8, 128), 1) // NZ

    def merge(pieces):
        cells = pieces[0][0]
        for piece, places in pieces[1:]:
            take = functools.reduce(jnp.logical_or, [group == p for p in places])
            cells = jnp.where(take, piece, cells)
        return cells

    def turned(piece, by):
        by = by * NZ % 128
        return pltpu.roll(piece, by, 1) if by else piece

    def pack_corner(planes, box, i, side, row_of):
        sign_x, sign_y = SENDS[side]
        lane = width - 128 if sign_y > 0 else 0
        height, places = corner_units(planes, sign_x, sign_y)
        for j, units in enumerate(places):
            for u, (k, n, m) in enumerate(units):
                stage[i, j, pl.ds(u, 1), :] = relaxed[k, pl.ds(row_of(n), 1), pl.ds(lane, 128)]
        for top in range(0, height, 8):
            pieces = []
            for j in range(4):
                m = 1 if j == 3 else 0
                own = GROUPS - 1 - m if sign_y > 0 else m
                pieces.append((turned(stage[i, j, pl.ds(top, 8), :], j - own), [j]))
            count = min(8, height - top)
            box[i, pl.ds(top, count), :] = merge(pieces)[:count]

    def pack_corners(planes, box):
        for i, (sign_x, _) in enumerate(SENDS[4:]):
            pack_corner(
                planes, box, i, 4 + i, (lambda n: rows - 1 - n) if sign_x > 0 else (lambda n: n)
            )

    def pack_rows(planes, box, i):
        sign = SENDS[i][0]
        for u, (k, n) in enumerate(row_units(planes, sign)):
            row = rows - 1 - n if sign > 0 else n
            for c in range(chunks):
                box[i, pl.ds(u * chunks + c, 1), :] = relaxed[
                    k, pl.ds(row, 1), pl.ds(c * 128, 128)
                ]

    def pack_columns(planes, box):
        for i, sign in enumerate((1, -1)):
            lane = width - 128 if sign > 0 else 0
            units = column_units(planes, sign)
            for t in range(0, len(units), GROUPS):
                parts = {}
                for place, (k, n) in enumerate(units[t : t + GROUPS]):
                    own = GROUPS - 1 - n if sign > 0 else n
                    parts.setdefault((k, place - own), []).append(place)
                for top in range(0, rows, 8):
                    box[i, pl.ds(t // GROUPS * rows + top, 8), :] = merge(
                        [
                            (turned(relaxed[k, pl.ds(top, 8), pl.ds(lane, 128)], by), places)
                            for (k, by), places in parts.items()
                        ]
                    )

    def unpack_rows(planes, box, i):
        sign = SENDS[i][0]
        for u, (k, n) in enumerate(row_units(planes, sign)):
            row = tall - 1 - n if sign > 0 else rows + n
            for c in range(chunks):
                relaxed[k, pl.ds(row, 1), pl.ds(c * 128, 128)] = box[
                    i, pl.ds(u * chunks + c, 1), :
                ]

    def unpack_columns(planes, box):
        for top in range(0, rows, 8):
            for k in range(planes):
                parts = {}
                for i, sign in enumerate((1, -1)):
                    units = column_units(planes, sign)
                    for n in range(layers_of(k, 1, sign)):
                        u = units.index((k, n))
                        own = GROUPS - 1 - n if sign > 0 else n
                        parts.setdefault((i, u // GROUPS, own - u % GROUPS), []).append(own)
                relaxed[k, pl.ds(top, 8), pl.ds(width, 128)] = merge(
                    [
                        (turned(box[i, pl.ds(t * rows + top, 8), :], by), places)
                        for (i, t, by), places in parts.items()
                    ]
                )

    def unpack_corners(planes, box):
        for i, (sign_x, sign_y) in enumerate(SENDS[4:]):
            height, places = corner_units(planes, sign_x, sign_y)
            for j, units in enumerate(places):
                m = 1 if j == 3 else 0
                own = GROUPS - 1 - m if sign_y > 0 else m
                for top in range(0, len(units), 8):
                    count = min(8, height - top)
                    stage[i, j, pl.ds(top, count), :] = turned(
                        box[i, pl.ds(top, count), :], own - j
                    )
                for u, (k, n, _) in enumerate(units):
                    row = tall - 1 - n if sign_x > 0 else rows + n
                    at = (k, pl.ds(row, 1), pl.ds(width, 128))
                    relaxed[at] = jnp.where(
                        group[:1] == own, stage[i, j, pl.ds(u, 1), :], relaxed[at]
                    )

    height = lax.broadcasted_iota(jnp.int32, (tall, wide), 1) % NZ

    near = lax.broadcasted_iota(jnp.int32, (8, wide), 1) % NZ
    edge = lax.broadcasted_iota(jnp.int32, (8, wide), 0)

    def pass_margin():
        last = pl.ds(rows - 8, 8)
        outer = pl.ds(rows, 8)
        first = pl.ds(0, 8)
        for k in range(POPS):
            step_x, step_y, step_z = MOVES[k]
            by = (step_y * NZ + step_z) % wide

            def along(at, k=k, by=by):
                return pltpu.roll(relaxed[k, at, :], by, 1) if by else relaxed[k, at, :]

            cells = along(outer)
            if step_x > 0:
                turn = pltpu.roll(cells, 1, 0)
                cells = jnp.where(edge == 0, pltpu.roll(along(last), 1, 0), turn)
                take = edge == 0
                if step_z:
                    take = take & (near != (0 if step_z == 1 else NZ - 1))
                state[k, first, :] = jnp.where(take, turn, state[k, first, :])
            elif step_x < 0:
                turn = pltpu.roll(cells, 7, 0)
                cells = jnp.where(edge == 7, pltpu.roll(along(first), 7, 0), turn)
                take = edge == 7
                if step_z:
                    take = take & (near != (0 if step_z == 1 else NZ - 1))
                state[k, last, :] = jnp.where(take, turn, state[k, last, :])
            if step_z:
                cells = jnp.where(
                    near == (0 if step_z == 1 else NZ - 1), relaxed[BACK[k], outer, :], cells
                )
            state[k, outer, :] = cells

    def carry_on(side):
        return pltpu.make_async_remote_copy(
            src_ref=passing.at[0],
            dst_ref=boxes[5].at[side - 4],
            send_sem=pass_sem,
            recv_sem=recv_sem.at[0, side],
            device_id=device(3),
            device_id_type=MESH,
        )

    def copies(step):
        x_out, x_got, y_out, y_got, c_out, c_got = boxes[6 * step : 6 * step + 6]
        pairs = []
        for side in range(8):
            if side < 2:
                source, target = x_out.at[side], x_got.at[side]
            elif side < 4:
                source, target = y_out.at[side - 2], y_got.at[side - 2]
            else:
                source, target = c_out.at[side - 4], c_got.at[side - 4]
            pairs.append(
                pltpu.make_async_remote_copy(
                    src_ref=source,
                    dst_ref=target,
                    send_sem=send_sem.at[step, side],
                    recv_sem=recv_sem.at[step, side],
                    device_id=device(side),
                    device_id_type=MESH,
                )
            )
        return pairs

    for step in range(ROUNDS):
        planes = POPS if step else PLANES
        x_out, x_got, y_out, y_got, c_out, c_got = boxes[6 * step : 6 * step + 6]
        sent = copies(step)
        last = rows // 8 - 1
        relax_row(upper * last, UNROLL)
        for index in range(1, last):
            relax_row(index, UNROLL)
        if step == 0:
            relax_row((1 - upper) * last, UNROLL)
            for side in (0, 1):
                pack_rows(planes, x_out, side)
            pack_columns(planes, y_out)
            pack_corners(planes, c_out)
            pl.semaphore_wait(barrier, jnp.where(plane == 0, 7, 8))
            for side in (0, 1):
                pl.when(upper == 1 - side)(sent[side].start)
            for side in (2, 3):
                sent[side].start()
            for side in range(4, 8):
                if first_out[side] is not None:
                    pl.when(first_out[side])(sent[side].start)
                else:
                    sent[side].start()
            for side in (0, 1):
                pl.when(upper == side)(sent[side].start)
        else:
            for side in (0, 1):

                @pl.when(upper == 1 - side)
                def _():
                    pack_rows(planes, x_out, side)
                    sent[side].start()

            relax_row((1 - upper) * last, UNROLL)
            pack_columns(planes, y_out)
            for side in (2, 3):
                sent[side].start()
            pack_corners(planes, c_out)
            for side in range(4, 8):
                sent[side].start()
            for side in (0, 1):

                @pl.when(upper == side)
                def _():
                    pack_rows(planes, x_out, side)
                    sent[side].start()

        if step == 0:
            for side in (0, 1):

                @pl.when((plane == 4) & (upper == side))
                def _():
                    sent[side].wait_recv()
                    unpack_rows(planes, x_got, side)
                    onward = 6 - side
                    pack_corner(
                        planes,
                        passing,
                        0,
                        onward,
                        (lambda n: tall - 1 - n) if side == 0 else (lambda n: rows + n),
                    )
                    carry_on(onward).start()

        for side in (2, 3):
            sent[side].wait_recv()
        unpack_columns(planes, y_got)
        for k in range(POPS):
            state[k, pl.ds(0, rows), :] = passed(relaxed, k, height)[:rows]
        for side in (4, 5, 6, 7):
            sent[side].wait_recv()
        unpack_corners(planes, c_got)
        for side in (0, 1):

            def take_rows(side=side):
                sent[side].wait_recv()
                unpack_rows(planes, x_got, side)

            if step == 0:
                pl.when(jnp.logical_not((plane == 4) & (upper == side)))(take_rows)
            else:
                take_rows()
        pass_margin()
        relax(tall // 8, wide // 128, UNROLL_ALL)
        if step < ROUNDS - 1:
            for k in range(POPS):
                state[k, pl.ds(0, rows), pl.ds(0, width)] = passed(relaxed, k, height)[
                    :rows, :width
                ]

    for step in range(ROUNDS):
        for side, copy in enumerate(copies(step)):
            if step == 0 and first_out[side] is not None:
                pl.when(first_out[side])(copy.wait_send)
            else:
                copy.wait_send()
    for side in (0, 1):
        pl.when((plane == 4) & (upper == side))(carry_on(6 - side).wait_send)


def passed(relaxed, k, height):
    step_x, step_y, step_z = MOVES[k]
    tall, wide = height.shape
    cells = relaxed[k]
    by = (step_y * NZ + step_z) % wide
    if by:
        cells = pltpu.roll(cells, by, 1)
    if step_x:
        cells = pltpu.roll(cells, step_x % tall, 0)
    if step_z:
        cells = jnp.where(height == (0 if step_z == 1 else NZ - 1), relaxed[BACK[k]], cells)
    return cells


def finish(relaxed, flow_out, trace_out, flow, trace, out_sem):
    rows, width = flow.shape[1:]
    height = lax.broadcasted_iota(jnp.int32, relaxed.shape[1:], 1) % NZ
    writes = []
    for k in range(POPS):
        near, far, at = (flow, flow_out, k) if k < FLOW else (trace, trace_out, k - FLOW)
        near[at] = passed(relaxed, k, height)[:rows, :width]
        writes.append(pltpu.make_async_copy(near.at[at], far.at[at], out_sem.at[k]))
        if k:
            writes[k - 1].start()
    writes[POPS - 1].start()
    for write in writes:
        write.wait()


def local(sizes, populations, tracer, solid_mask, inflow, wind_profile, emission):
    rows, width = solid_mask.shape
    chunks = width // 128
    tall, wide = rows + ROW_MARGIN, width + LANE_MARGIN
    far = pl.BlockSpec(memory_space=pltpu.HBM)
    near = pl.BlockSpec(memory_space=pltpu.VMEM)
    boxes = []
    for step in range(ROUNDS):
        kind = 1 if step else 0
        for shape in (
            (2, ROWS_OF[kind] * chunks, 128),
            (2, TILES_OF[kind] * rows, 128),
            (4, CORNER_OF[kind], 128),
        ):
            boxes += [pltpu.VMEM(shape, jnp.float32)] * 2
    held_far = [
        pltpu.with_memory_space_constraint(a, pltpu.HBM)
        for a in (populations, tracer, solid_mask, inflow, wind_profile, emission)
    ]
    relaxed = pl.pallas_call(
        functools.partial(exchange, sizes),
        out_shape=pltpu.VMEM((PLANES, tall, wide), jnp.float32),
        in_specs=[far] * 6,
        out_specs=near,
        scratch_shapes=[
            pltpu.VMEM((POPS, tall, wide), jnp.float32),
            pltpu.VMEM((rows, width), jnp.int32),
            pltpu.VMEM((rows, width), jnp.int32),
            pltpu.VMEM(wind_profile.shape, jnp.float32),
            pltpu.VMEM((FLOW, 8, 128), jnp.float32),
            pltpu.VMEM((4, 4, 16, 128), jnp.float32),
            pltpu.SemaphoreType.DMA((6,)),
            pltpu.SemaphoreType.DMA((ROUNDS, 8)),
            pltpu.SemaphoreType.DMA((ROUNDS, 8)),
            pltpu.VMEM((1, CORNER_OF[0], 128), jnp.float32),
            pltpu.SemaphoreType.DMA,
            *boxes,
        ],
        compiler_params=pltpu.CompilerParams(
            collective_id=0, has_side_effects=True, vmem_limit_bytes=24 << 20
        ),
        name="exchange",
    )(*held_far)
    return pl.pallas_call(
        finish,
        out_shape=(
            jax.ShapeDtypeStruct(populations.shape, jnp.float32),
            jax.ShapeDtypeStruct(tracer.shape, jnp.float32),
        ),
        in_specs=[near],
        out_specs=(far, far),
        scratch_shapes=[
            pltpu.VMEM(populations.shape, jnp.float32),
            pltpu.VMEM(tracer.shape, jnp.float32),
            pltpu.SemaphoreType.DMA((POPS,)),
        ],
        compiler_params=pltpu.CompilerParams(vmem_limit_bytes=16 << 20),
        name="finish",
    )(pltpu.with_memory_space_constraint(relaxed, pltpu.VMEM))


def solution(mesh):
    sizes = (mesh.shape["gx"], mesh.shape["gy"])
    in_specs = (
        P(None, "gx", "gy"),
        P(None, "gx", "gy"),
        P("gx", "gy"),
        P("gx", "gy"),
        P(),
        P("gx", "gy"),
    )
    out_specs = (P(None, "gx", "gy"), P(None, "gx", "gy"))
    return jax.shard_map(
        functools.partial(local, sizes),
        mesh=mesh,
        in_specs=in_specs,
        out_specs=out_specs,
        check_vma=False,
    )
```
